32 devices in a mesh: gx: 2 (over x), gy: 4 (over y, core), gz: 4 (over z).
Axes of the slice: x: 2, y: 2, z: 4, core: 2. Of those that a mesh axis runs over, the one named last changes fastest.
Arguments:
- positions: float32 [3, 32768], P(None, ('gx', 'gy', 'gz')), may hold values from 0 to 16, as said below
- velocities: float32 [3, 32768], P(None, ('gx', 'gy', 'gz')), may hold values from -6 to 6
- inv_mass: float32 [32768], P(('gx', 'gy', 'gz')), may hold values from 0.5 to 2
- charge: float32 [32768], P(('gx', 'gy', 'gz')), may hold values from -4 to 4
- fast_force: float32 [3, 32768], P(None, ('gx', 'gy', 'gz')), may hold values from -6 to 6
- slow_force: float32 [3, 32768], P(None, ('gx', 'gy', 'gz')), may hold values from -6 to 6
- bonds: int32 [2, 32768], P(None, ('gx', 'gy', 'gz')), may hold values from 0 to 1023
- bond_k: float32 [32768], P(('gx', 'gy', 'gz')), may hold values from 0.05 to 0.4
- halo_index: int32 [6, 8192], P(None, ('gx', 'gy', 'gz')), may hold values from 0 to 1023
- pair_own: int32 [3072], P(('gx', 'gy', 'gz')), may hold values from 0 to 7
- pair_partner: int32 [3072], P(('gx', 'gy', 'gz')), may hold values from 0 to 19
- pair_count: int32 [32], P(('gx', 'gy', 'gz')), may hold values from 1 to 96
Outputs:
- displacement: float32 [3, 32768], P(None, ('gx', 'gy', 'gz'))
- velocities_out: float32 [3, 32768], P(None, ('gx', 'gy', 'gz'))
- fast_out: float32 [3, 32768], P(None, ('gx', 'gy', 'gz'))
- slow_out: float32 [3, 32768], P(None, ('gx', 'gy', 'gz'))
The draws below stay inside these ranges and needn't reach their ends.
Inputs may be any that keep to these rules, and one draw needn't show every extreme that they name: `positions`: atoms of patch p lie in the cube of side 4 at 4 times its grid place.
All inputs are finite; a program needn't handle non-finite values.
Results may differ from the reference program's by a relative error of at most 0.0003.
Values sent between devices are 32-bit elements; how exact they have to be, the bound alone decides.
No kernel may reach another device: no remote copies, remote signals or barrier semaphores. Data moves between devices by JAX's collectives and lax.ppermute only.
A program may use at most 64 MiB of HBM per device.

```python
import math
import jax
import jax.numpy as jnp
from jax import lax

ATOMS_DEV = 1024
HALO = 256
INNER = 4
PER_PEER = 6
ATOMS = 32768
TILES_DEV = 8
PARTNERS = 20
PAIR_SLOTS = 96
NBONDS = 1024
N_GX = 2
N_GY = 4
N_GZ = 4
DEVICES = 32


patch_side = 4.0


face_margin = 1.0


def face_slots(key):
    patches = N_GX * N_GY * N_GZ
    return jax.random.randint(jax.random.fold_in(key, 11), (6, patches * HALO), 0, ATOMS_DEV).astype(jnp.int32)


def draw_halo_index(key, part):
    return face_slots(key)


def draw_positions(key, part):
    patches = N_GX * N_GY * N_GZ
    inside = jax.random.uniform(jax.random.fold_in(key, 3), (3, patches, ATOMS_DEV), jnp.float32, 0.0, patch_side)
    depth = jax.random.uniform(jax.random.fold_in(key, 5), (6, patches, HALO), jnp.float32, 0.0, face_margin)
    slots = face_slots(key).reshape(6, patches, HALO)
    patch_rows = jnp.arange(patches)[:, None]
    for face_id in range(6):
        axis_id = face_id // 2
        if face_id % 2 == 0:
            placed = depth[face_id]
        else:
            placed = patch_side - depth[face_id]
        inside = inside.at[axis_id, patch_rows, slots[face_id]].set(placed)
    patch_ids = jnp.arange(patches)
    anchor = jnp.stack([patch_ids // (N_GY * N_GZ), patch_ids // N_GZ % N_GY, patch_ids % N_GZ]).astype(jnp.float32)
    return (inside + patch_side * anchor[:, :, None]).reshape(3, patches * ATOMS_DEV)


def with_ends(drawn, stream_key, smallest, top_value):
    extent = drawn.shape
    index_at = [jax.random.randint(jax.random.fold_in(stream_key, axis), (), 0, extent[axis]) for axis in range(len(extent))]
    drawn = drawn.at[tuple(index_at)].set(smallest)
    longest = extent.index(max(extent))
    index_at[longest] = (index_at[longest] + 1) % extent[longest]
    return drawn.at[tuple(index_at)].set(top_value)


def steps_of(rng, extent, split, least, top_value):
    def one(position, blocks):
        draws = jax.random.uniform(jax.random.fold_in(jax.random.fold_in(rng, 6), position), (blocks,), jnp.float32, least / len(split), top_value / len(split))
        return jnp.repeat(jnp.exp(draws), extent[position] // blocks).reshape((-1,) + (1,) * (len(extent) - position - 1))

    gain = one(*split[0])
    for cut in split[1:]:
        gain = gain * one(*cut)
    return gain


def normal_values(key, shape, width, reach, cuts=(), dtype=jnp.bfloat16):
    entries = jax.random.normal(key, shape, jnp.float32) * width
    if len(cuts) > 0:
        entries = steps_of(key, shape, cuts, -0.22, 0.18) * entries
    return jnp.clip(entries, min=-reach, max=reach).astype(dtype)


def setup_inputs(seed: int = 0) -> dict:
    seeds = jax.random.split(jax.random.key(seed), 13)
    return {
        "positions": draw_positions(jax.random.fold_in(seeds[12], 71), 0),
        "velocities": normal_values(seeds[1], (3, ATOMS), 1.0, 6.0, ((1, 32),), jnp.float32),
        "inv_mass": jnp.clip(jnp.exp(math.log(2.0) - 1.3862944 * jax.random.uniform(seeds[2], (ATOMS,), jnp.float32) ** steps_of(seeds[2], (ATOMS,), ((0, 32),), -0.2, 0.2)), 0.5, 2.0),
        "charge": normal_values(seeds[3], (ATOMS,), 1.0, 4.0, ((0, 32),), jnp.float32),
        "fast_force": normal_values(seeds[4], (3, ATOMS), 1.0, 6.0, ((1, 32),), jnp.float32),
        "slow_force": normal_values(seeds[5], (3, ATOMS), 1.0, 6.0, ((1, 32),), jnp.float32),
        "bonds": with_ends(jax.random.randint(seeds[6], (2, NBONDS * DEVICES), 0, ATOMS_DEV), jax.random.fold_in(seeds[6], 1), 0, ATOMS_DEV - 1).astype(jnp.int32),
        "bond_k": jnp.clip(jnp.exp(math.log(0.4) - 2.0794415 * jax.random.uniform(seeds[7], (NBONDS * DEVICES,), jnp.float32) ** steps_of(seeds[7], (NBONDS * DEVICES,), ((0, 32),), -0.2, 0.2)), 0.05, 0.4),
        "halo_index": draw_halo_index(jax.random.fold_in(seeds[12], 71), 0),
        "pair_own": with_ends(jax.random.randint(seeds[9], (PAIR_SLOTS * DEVICES,), 0, TILES_DEV), jax.random.fold_in(seeds[9], 1), 0, TILES_DEV - 1).astype(jnp.int32),
        "pair_partner": with_ends(jax.random.randint(seeds[10], (PAIR_SLOTS * DEVICES,), 0, PARTNERS), jax.random.fold_in(seeds[10], 1), 0, PARTNERS - 1).astype(jnp.int32),
        "pair_count": with_ends(jax.random.randint(seeds[11], (DEVICES,), 1, PAIR_SLOTS + 1), jax.random.fold_in(seeds[11], 1), 1, PAIR_SLOTS).astype(jnp.int32),
    }


step_inner = 0.1
short_scale = 1.0
short_reach = 0.64
long_scale = 0.5
long_reach = 1.44


def short_block(row_piece, others, weight):
    separation = row_piece[:, :, None] - others[:, None, :]
    nearness = jnp.maximum(1.0 - jnp.sum(separation * separation, axis=0) / short_reach, 0.0) * weight[None, :]
    return short_scale * jnp.sum(separation * nearness[None], axis=2)


def short_force(own, others, weight):
    row_count = own.shape[1]
    block_rows = min(512, row_count)
    pieces = own.reshape(3, row_count // block_rows, block_rows).transpose(1, 0, 2)
    result = lax.map(lambda row_piece: short_block(row_piece, others, weight), pieces)
    return result.transpose(1, 0, 2).reshape(3, row_count)


def tile_force(packet):
    separation = packet[0:3, :, None] - packet[4:7, None, :]
    nearness = jnp.maximum(1.0 - jnp.sum(separation * separation, axis=0) / long_reach, 0.0) * packet[7][None, :]
    return long_scale * packet[3][None, :] * jnp.sum(separation * nearness[None], axis=2)


def block_forces(packets):
    return lax.map(lambda source_group: jax.vmap(tile_force)(source_group), packets)


def from_lower(block_data, dimension):
    edge = jnp.zeros_like(lax.slice_in_dim(block_data, 0, 1, axis=dimension))
    kept = lax.slice_in_dim(block_data, 0, block_data.shape[dimension] - 1, axis=dimension)
    return jnp.concatenate([edge, kept], axis=dimension)


def from_upper(block_data, dimension):
    edge = jnp.zeros_like(lax.slice_in_dim(block_data, 0, 1, axis=dimension))
    kept = lax.slice_in_dim(block_data, 1, block_data.shape[dimension], axis=dimension)
    return jnp.concatenate([kept, edge], axis=dimension)


def bonded_all(current, bonds, bond_k):
    offsets = ((jnp.arange(bonds.shape[1]) // ATOMS_DEV) * ATOMS_DEV).astype(jnp.int32)
    first = bonds[0].astype(jnp.int32) + offsets
    second = bonds[1].astype(jnp.int32) + offsets
    bond_pull = bond_k[None, :] * (current[:, first] - current[:, second])
    zero_force = jnp.zeros_like(current)
    return zero_force.at[:, first].add(-bond_pull).at[:, second].add(bond_pull)


def fast_all(current, charge, bonds, bond_k, halo_index):
    patches = N_GX * N_GY * N_GZ
    stacked = jnp.concatenate([current, charge[None, :]], axis=0)
    grid = stacked.reshape(4, N_GX, N_GY, N_GZ, ATOMS_DEV)
    index_grid = halo_index.reshape(6, N_GX, N_GY, N_GZ, HALO)
    faces = []
    for face_id in range(6):
        wide_index = jnp.broadcast_to(index_grid[face_id][None], (4, N_GX, N_GY, N_GZ, HALO))
        faces.append(jnp.take_along_axis(grid, wide_index, axis=4))
    unit = jnp.ones((1, N_GX, N_GY, N_GZ, HALO), jnp.float32)
    pieces = [grid]
    marks = [jnp.ones((1, N_GX, N_GY, N_GZ, ATOMS_DEV), jnp.float32)]
    for axis_id in range(3):
        dimension = axis_id + 1
        pieces.append(from_lower(faces[2 * axis_id + 1], dimension))
        pieces.append(from_upper(faces[2 * axis_id], dimension))
        marks.append(from_lower(unit, dimension))
        marks.append(from_upper(unit, dimension))
    others = jnp.concatenate(pieces, axis=4).reshape(4, patches, -1).transpose(1, 0, 2)
    weight = jnp.concatenate(marks, axis=4).reshape(patches, -1)
    own = current.reshape(3, patches, ATOMS_DEV).transpose(1, 0, 2)
    short = lax.map(lambda item: short_force(item[0], item[1][:3], item[2]), (own, others, weight))
    short = short.transpose(1, 0, 2).reshape(3, -1)
    return short + bonded_all(current, bonds, bond_k), stacked, others


def slow_all(stacked, others, pair_own, pair_partner, pair_count):
    patches = N_GX * N_GY * N_GZ
    slot_count = pair_own.shape[0] // patches
    tile_count = ATOMS_DEV // 128
    own_tiles = stacked.reshape(4, patches, tile_count, 128).transpose(1, 2, 0, 3)
    partners = others.reshape(patches, 4, -1, 128).transpose(0, 2, 1, 3)
    own_index = pair_own.reshape(patches, slot_count).astype(jnp.int32)
    partner_index = pair_partner.reshape(patches, slot_count).astype(jnp.int32)
    own_rows = jax.vmap(lambda tiles_of, chosen: tiles_of[chosen])(own_tiles, own_index)
    partner_rows = jax.vmap(lambda tiles_of, chosen: tiles_of[chosen])(partners, partner_index)
    live_slots = (jnp.arange(slot_count)[None, :] < pair_count[:, None]).astype(jnp.float32)
    packets = jnp.concatenate([own_rows[:, :, :3], own_rows[:, :, 3:] * live_slots[:, :, None, None], partner_rows], axis=2)
    tile_terms = lax.map(lambda patch_packets: block_forces(patch_packets.reshape(-1, PER_PEER, 8, 128)).reshape(-1, 3, 128), packets)
    select = (own_index[:, :, None] == jnp.arange(tile_count)[None, None, :]).astype(jnp.float32)
    slow_now = jnp.einsum("pst,psck->cptk", select, tile_terms, precision=lax.Precision.HIGHEST)
    return slow_now.reshape(3, -1)


def reference(positions, velocities, inv_mass, charge, fast_force, slow_force, bonds, bond_k, halo_index, pair_own, pair_partner, pair_count):
    half_inner = 0.5 * step_inner
    half_outer = 0.5 * INNER * step_inner
    moving = velocities + half_outer * inv_mass[None, :] * slow_force
    current = positions
    force_now = fast_force
    for inner_turn in range(INNER):
        moving = moving + half_inner * inv_mass[None, :] * force_now
        current = current + step_inner * moving
        force_now, stacked, others = fast_all(current, charge, bonds, bond_k, halo_index)
        moving = moving + half_inner * inv_mass[None, :] * force_now
    slow_now = slow_all(stacked, others, pair_own, pair_partner, pair_count)
    moving = moving + half_outer * inv_mass[None, :] * slow_now
    return current - positions, moving, force_now, slow_now
```

```python
import functools

import jax
import jax.numpy as jnp
from jax import lax
from jax.experimental import pallas as pl
from jax.experimental.pallas import tpu as pltpu
from jax.sharding import PartitionSpec as P

AXES = ("gx", "gy", "gz")
INNER = 4
STEP = 0.1
SHORT_REACH = 0.64
LONG_REACH = 1.44
LONG_SCALE = 0.5
SIDE = 4.0
INV_LEN = 1.25
LEN = 0.8
LANES = 128
BLOCK = 256
FAR = -1.0e6
MAGIC = 32768.0

F32 = jnp.float32
BF16 = jnp.bfloat16


def matchings(sizes):
    nx, ny, nz = sizes
    assert nx % 2 == 0 and ny % 2 == 0 and nz % 2 == 0
    swaps = []
    for axis in (2, 0, 1):
        for phase in range(1 if sizes[axis] == 2 else 2):
            perm = []
            for a in range(nx):
                for b in range(ny):
                    for c in range(nz):
                        place = [a, b, c]
                        p = place[axis]
                        partner = p ^ 1 if phase == 0 else (p + 1 if p % 2 else p - 1)
                        if 0 <= partner < sizes[axis]:
                            place[axis] = partner
                        else:
                            other = 0 if axis == 1 else 1
                            place[other] ^= 1
                        perm.append(
                            ((a * ny + b) * nz + c, (place[0] * ny + place[1]) * nz + place[2])
                        )
            swaps.append((axis, phase, perm))
    return swaps


def rounded(a):
    return a.astype(BF16).astype(F32)


def split3(a):
    high = rounded(a)
    rest = a - high
    mid = rounded(rest)
    return high, mid, rounded(rest - mid)


def row_ids(shape):
    return lax.broadcasted_iota(jnp.int32, shape, 0)


def pick_rows(rows, shape):
    ids = row_ids(shape)
    out = jnp.zeros(shape, F32)
    for s, r in enumerate(rows):
        out = jnp.where(ids == s, r, out)
    return out


def centre(shape):
    parts = [lax.axis_index(ax).astype(F32) * SIDE + 0.5 * SIDE for ax in AXES]
    return pick_rows(parts, shape)


def scaled(x, mid):
    n = x.shape[1]
    full = jnp.concatenate([x[:3], jnp.zeros((5, n), F32)], axis=0)
    return (full - mid) * INV_LEN


def receiver_matrix(u):
    h, m, l = split3(u)
    norm = 1.0 - jnp.sum(u * u, axis=0, keepdims=True)
    a, b, c = split3(norm)
    h, m, l = 2.0 * h, 2.0 * m, 2.0 * l
    one = jnp.ones_like(norm)
    tail = pick_rows([a, b, c, one, one, one], u.shape)
    return jnp.concatenate([h, h, h, m, m, l, tail, jnp.zeros_like(u)], axis=0).astype(BF16)


def source_matrices(u, valid=None):
    h, m, l = split3(u)
    norm = -jnp.sum(u * u, axis=0, keepdims=True)
    if valid is not None:
        norm = jnp.where(valid, norm, FAR)
    a, b, c = split3(norm)
    one = jnp.ones_like(norm)
    tail = pick_rows([one, one, one, a, b, c], u.shape)
    pair = jnp.concatenate([h, m, l, h, m, h, tail, jnp.zeros_like(u)], axis=0)
    ids = row_ids(u.shape)
    total = jnp.concatenate([jnp.where(ids == 3, 1.0, h), m, l], axis=0).astype(BF16)
    return pair, total


def dot(a, b):
    return jnp.dot(a, b, preferred_element_type=F32)


def two_parts(w):
    high = (w + MAGIC) - MAGIC
    return high.astype(BF16), (w - high).astype(BF16)


def gather_lanes(sources, index):
    index = jnp.broadcast_to(index, (8, LANES))
    tile = lax.shift_right_logical(index, 7)
    lane = lax.bitwise_and(index, LANES - 1)
    out = jnp.zeros((8, LANES), F32)
    for r, src in enumerate(sources):
        out = jnp.where(tile == r, jnp.take_along_axis(src, lane, axis=1), out)
    return out


def lane_tiles(a):
    return [a[:, r * LANES : (r + 1) * LANES] for r in range(a.shape[1] // LANES)]


def pad8(x):
    return jnp.concatenate([x, jnp.zeros((8 - x.shape[0], x.shape[1]), F32)], axis=0)


def write_faces(swaps, x, charge, index_ref, send_refs):
    rows = [x] if charge is None else [x, charge]
    tiles = lane_tiles(pad8(jnp.concatenate(rows, axis=0)))
    for (axis, phase, _), ref in zip(swaps, send_refs):
        even = lax.axis_index(AXES[axis]) % 2 == 0
        high = even if phase == 0 else jnp.logical_not(even)
        index = jnp.where(high, index_ref[2 * axis + 1 : 2 * axis + 2, :], index_ref[2 * axis : 2 * axis + 1, :])
        for w in range(index.shape[1] // LANES):
            part = slice(w * LANES, (w + 1) * LANES)
            ref[:, part] = gather_lanes(tiles, index[:, part])[:4]


def start_kernel(swaps, x_ref, v_ref, mass_ref, fast_ref, slow_ref, index_ref, x_out, v_out, *send_refs):
    mass = mass_ref[...]
    v = v_ref[...] + (0.5 * INNER * STEP) * mass * slow_ref[...]
    v = v + (0.5 * STEP) * mass * fast_ref[...]
    x = x_ref[...] + STEP * v
    x_out[...] = x
    v_out[...] = v
    write_faces(swaps, x, None, index_ref, send_refs)


def pair_sums(receivers, sources, totals, slow_totals, sums, slow_sums):
    for it in range(len(receivers)):
        for st in range(len(sources)):
            closeness = dot(sources[st], receivers[it])
            high, low = two_parts(jnp.maximum(closeness, 0.0))
            sums[it] = sums[it] + (dot(totals[st], high) + dot(totals[st], low))
            if slow_totals is not None:
                ratio = SHORT_REACH / LONG_REACH
                wide = jnp.maximum(closeness * ratio + (1.0 - ratio), 0.0)
                high, low = two_parts(wide)
                lhs = slow_totals[it][st]
                slow_sums[it] = slow_sums[it] + (dot(lhs, high) + dot(lhs, low))


def short_from(u, sums):
    part = sums[0:8] + sums[8:16] + sums[16:24]
    return LEN * (u * part[3:4] - part)


def blocks(a, width=BLOCK):
    return [a[:, s : s + width] for s in range(0, a.shape[1], width)]


def tile_counts(own_ref, partner_ref, count_ref, n_tiles, swaps):
    slots = own_ref.shape[1]
    partner = partner_ref[...]
    own = own_ref[...]
    live = lax.broadcasted_iota(jnp.int32, (1, slots), 1) < count_ref[0]
    outside = partner - n_tiles
    axis = lax.shift_right_logical(outside, 2)
    side = lax.bitwise_and(lax.shift_right_logical(outside, 1), 1)
    within = lax.bitwise_and(outside, 1)
    place = jnp.full_like(partner, -1)
    for k, (ax, phase, _) in enumerate(swaps):
        even = lax.axis_index(AXES[ax]) % 2 == 0
        high = even if phase == 0 else jnp.logical_not(even)
        want = jnp.where(high, 1, 0)
        place = jnp.where((axis == ax) & (side == want), n_tiles + 2 * k + within, place)
    place = jnp.where(outside < 0, partner, place)
    own_hot = jnp.where((row_ids((8, slots)) == own) & live, 1.0, 0.0)
    place_hot = jnp.where(row_ids((32, slots)) == place, 1.0, 0.0)
    return lax.dot_general(own_hot, place_hot, (((1,), (1,)), ((), ())), preferred_element_type=F32)


def slow_matrices(u, charge, counts, first_tile):
    n = u.shape[1]
    ids = row_ids(u.shape)
    base = jnp.where(ids == 3, 1.0, u) * charge
    wide = []
    for t in range(8):
        per = [
            jnp.broadcast_to(counts[t : t + 1, first_tile + w : first_tile + w + 1], (1, LANES))
            for w in range(n // LANES)
        ]
        wide.append(jnp.concatenate(per, axis=1))
    out = []
    for it in range(4):
        parts = []
        for t in (2 * it, 2 * it + 1):
            parts.extend(split3(base * wide[t]))
        out.append(jnp.concatenate(parts, axis=0).astype(BF16))
    return out


def slow_from(u, charge, sums):
    low = sums[0:8] + sums[8:16] + sums[16:24]
    high = sums[24:32] + sums[32:40] + sums[40:48]
    part = jnp.concatenate([low[:, :LANES], high[:, LANES:]], axis=1)
    return (LONG_SCALE * LEN) * charge * (u * part[3:4] - part)


def own_kernel(swaps, first, last, *refs):
    refs = list(refs)
    x_ref, bonds_ref, bond_k_ref = refs[:3]
    refs = refs[3:]
    if not first:
        incidence = refs.pop(0)
    if last:
        charge_ref, own_ref, partner_ref, count_ref = refs[:4]
        refs = refs[4:]
    out_ref = refs.pop(0)
    if first:
        incidence = refs.pop(0)
    if last:
        slow_ref = refs.pop(0)
    x = x_ref[...]
    n = x.shape[1]
    tiles = lane_tiles(pad8(x))
    pulls = []
    for t in range(n // LANES):
        part = slice(t * LANES, (t + 1) * LANES)
        gap = gather_lanes(tiles, bonds_ref[0:1, part]) - gather_lanes(tiles, bonds_ref[1:2, part])
        pulls.append(bond_k_ref[:, part] * gap)
    pull = jnp.concatenate(pulls, axis=1)
    pull = jnp.concatenate(split3(pull), axis=0).astype(BF16)
    if first:
        for t in range(n // LANES):
            part = slice(t * LANES, (t + 1) * LANES)
            i = jnp.transpose(jnp.broadcast_to(bonds_ref[0:1, part], (LANES, LANES)))
            j = jnp.transpose(jnp.broadcast_to(bonds_ref[1:2, part], (LANES, LANES)))
            for s in range(n // LANES):
                atom = lax.broadcasted_iota(jnp.int32, (LANES, LANES), 1) + s * LANES
                hit = jnp.where(j == atom, 1.0, 0.0)
                hit = jnp.where(i == atom, hit - 1.0, hit)
                incidence[part, s * LANES : (s + 1) * LANES] = hit.astype(BF16)
    bonded = dot(pull, incidence[...])
    bonded = bonded[0:8] + bonded[8:16] + bonded[16:24]

    u = scaled(x, centre((8, n)))
    receivers = blocks(receiver_matrix(u))
    pair, total = source_matrices(u)
    sources = [jnp.transpose(p).astype(BF16) for p in blocks(pair)]
    totals = blocks(total)
    count = len(receivers)
    sums = [jnp.zeros((24, BLOCK), F32)] * count
    slow_totals = slow_sums = None
    if last:
        counts = tile_counts(own_ref, partner_ref, count_ref, n // LANES, swaps)
        per_source = [
            slow_matrices(b, q, counts, s * (BLOCK // LANES))
            for s, (b, q) in enumerate(zip(blocks(u), blocks(charge_ref[...])))
        ]
        slow_totals = [[per_source[s][it] for s in range(len(sources))] for it in range(count)]
        slow_sums = [jnp.zeros((48, BLOCK), F32)] * count
    pair_sums(receivers, sources, totals, slow_totals, sums, slow_sums)
    force = short_from(u, jnp.concatenate(sums, axis=1)) + bonded
    out_ref[...] = force[:3]
    if last:
        slow = [
            slow_from(b, q, s) for b, q, s in zip(blocks(u), blocks(charge_ref[...]), slow_sums)
        ]
        slow_ref[...] = jnp.concatenate(slow, axis=1)[:3]


def halo_kernel(swaps, last, send_charge, *refs):
    refs = list(refs)
    x_ref, v_ref, mass_ref, force_ref = refs[:4]
    refs = refs[4:]
    arrived = refs[: len(swaps)]
    refs = refs[len(swaps) :]
    if last:
        charge_ref, own_ref, partner_ref, count_ref, slow_ref, start_ref = refs[:6]
        moved_out, v_out, force_out, slow_out = refs[6:]
    else:
        index_ref = refs.pop(0)
        if send_charge:
            charge_ref = refs.pop(0)
        x_out, v_out = refs[:2]
        send_refs = refs[2:]
    x = x_ref[...]
    n = x.shape[1]
    u = scaled(x, centre((8, n)))
    receivers = blocks(receiver_matrix(u))
    count = len(receivers)
    mid = centre((8, BLOCK))
    sources, totals, slow_totals = [], [], [[] for _ in range(count)] if last else None
    if last:
        counts = tile_counts(own_ref, partner_ref, count_ref, n // LANES, swaps)
    for k, ((axis, phase, _), ref) in enumerate(zip(swaps, arrived)):
        place = lax.axis_index(AXES[axis])
        if phase == 0:
            valid = place >= 0
        else:
            valid = (place > 0) & (place < lax.axis_size(AXES[axis]) - 1)
        got = ref[...]
        there = jnp.where(valid, scaled(got, mid), 0.0)
        pair, total = source_matrices(there, valid)
        sources.append(jnp.transpose(pair).astype(BF16))
        totals.append(total)
        if last:
            per = slow_matrices(there, got[3:4], counts, n // LANES + k * (BLOCK // LANES))
            for it in range(count):
                slow_totals[it].append(per[it])
    sums = [jnp.zeros((24, BLOCK), F32)] * count
    slow_sums = [jnp.zeros((48, BLOCK), F32)] * count
    pair_sums(receivers, sources, totals, slow_totals, sums, slow_sums)
    mass = mass_ref[...]
    force = force_ref[...] + short_from(u, jnp.concatenate(sums, axis=1))[:3]
    v = v_ref[...] + (0.5 * STEP) * mass * force
    if last:
        slow = [
            slow_from(b, q, s) for b, q, s in zip(blocks(u), blocks(charge_ref[...]), slow_sums)
        ]
        slow = slow_ref[...] + jnp.concatenate(slow, axis=1)[:3]
        v_out[...] = v + (0.5 * INNER * STEP) * mass * slow
        moved_out[...] = x - start_ref[...]
        force_out[...] = force
        slow_out[...] = slow
    else:
        v = v + (0.5 * STEP) * mass * force
        x = x + STEP * v
        x_out[...] = x
        v_out[...] = v
        write_faces(swaps, x, charge_ref[...] if send_charge else None, index_ref, send_refs)


def call(kernel, outs, args, smem=(), flops=0):
    specs = [
        pl.BlockSpec(memory_space=pltpu.SMEM if i in smem else pltpu.VMEM) for i in range(len(args))
    ]
    return pl.pallas_call(
        kernel,
        out_shape=[jax.ShapeDtypeStruct(s, d) for s, d in outs],
        in_specs=specs,
        out_specs=[pl.BlockSpec(memory_space=pltpu.VMEM)] * len(outs),
        compiler_params=pltpu.CompilerParams(vmem_limit_bytes=24 * 1024 * 1024),
        cost_estimate=pl.CostEstimate(flops=flops, bytes_accessed=100000, transcendentals=0),
    )(*args)


def on_device(
    swaps,
    positions,
    velocities,
    inv_mass,
    charge,
    fast_force,
    slow_force,
    bonds,
    bond_k,
    halo_index,
    pair_own,
    pair_partner,
    pair_count,
):
    n = positions.shape[1]
    width = halo_index.shape[1]
    mass = inv_mass.reshape(1, n)
    charge = charge.reshape(1, n)
    bond_k = bond_k.reshape(1, -1)
    own = pair_own.reshape(1, -1)
    partner = pair_partner.reshape(1, -1)
    vec = ((3, n), F32)
    sends = [((4, width), F32)] * len(swaps)
    x, v, *faces = call(
        functools.partial(start_kernel, swaps),
        [vec, vec] + sends,
        [positions, velocities, mass, fast_force, slow_force, halo_index],
    )
    incidence = None
    for turn in range(INNER):
        first, last = turn == 0, turn == INNER - 1
        arrived = [lax.ppermute(f, AXES, perm) for f, (_, _, perm) in zip(faces, swaps)]
        outs = [vec]
        args = [x, bonds, bond_k]
        smem = ()
        if first:
            outs.append(((bonds.shape[1], n), BF16))
        else:
            args.append(incidence)
        if last:
            args += [charge, own, partner, pair_count]
            smem = (len(args) - 1,)
            outs.append(vec)
        got = call(
            functools.partial(own_kernel, swaps, first, last), outs, args, smem, flops=2 * 10**9
        )
        force = got[0]
        if first:
            incidence = got[1]
        args = [x, v, mass, force] + arrived
        if last:
            args += [charge, own, partner, pair_count, got[-1], positions]
            moved, v, force, slow = call(
                functools.partial(halo_kernel, swaps, True, False),
                [vec] * 4,
                args,
                (len(args) - 3,),
                flops=10**9,
            )
            return moved, v, force, slow
        send_charge = turn == INNER - 2
        args.append(halo_index)
        if send_charge:
            args.append(charge)
        x, v, *faces = call(
            functools.partial(halo_kernel, swaps, False, send_charge),
            [vec, vec] + sends,
            args,
            flops=10**9,
        )


def solution(mesh):
    rows = P(None, AXES)
    flat = P(AXES)
    swaps = matchings([mesh.shape[ax] for ax in AXES])
    return jax.shard_map(
        functools.partial(on_device, swaps),
        mesh=mesh,
        in_specs=(rows, rows, flat, flat, rows, rows, rows, flat, rows, flat, flat, flat),
        out_specs=(rows, rows, rows, rows),
        check_vma=False,
    )
```

```python
import functools

import jax
import jax.numpy as jnp
from jax import lax
from jax.experimental import pallas as pl
from jax.experimental.pallas import tpu as pltpu
from jax.sharding import PartitionSpec as P

AXES = ("gx", "gy", "gz")
INNER = 4
STEP = 0.1
LONG_SCALE = 0.5
SIDE = 4.0
SHORT_UNIT = 0.8
LONG_UNIT = 1.2
LANES = 128
BLOCK = 256
FAR = -1.0e6

N_START = 12
F32 = jnp.float32
BF16 = jnp.bfloat16


def matchings(sizes):
    nx, ny, nz = sizes
    assert nx % 2 == 0 and ny % 2 == 0 and nz % 2 == 0
    swaps = []
    for axis in (2, 0, 1):
        for phase in range(1 if sizes[axis] == 2 else 2):
            perm = []
            for a in range(nx):
                for b in range(ny):
                    for c in range(nz):
                        place = [a, b, c]
                        p = place[axis]
                        partner = p ^ 1 if phase == 0 else (p + 1 if p % 2 else p - 1)
                        if 0 <= partner < sizes[axis]:
                            place[axis] = partner
                        else:
                            other = 0 if axis == 1 else 1
                            place[other] ^= 1
                        perm.append(
                            ((a * ny + b) * nz + c, (place[0] * ny + place[1]) * nz + place[2])
                        )
            swaps.append((axis, phase, perm))
    return swaps


def rounded(a):
    return a.astype(BF16).astype(F32)


def split3(a):
    high = rounded(a)
    rest = a - high
    mid = rounded(rest)
    return high, mid, rounded(rest - mid)


def row_ids(shape):
    return lax.broadcasted_iota(jnp.int32, shape, 0)


def pick_rows(rows, shape):
    ids = row_ids(shape)
    out = jnp.zeros(shape, F32)
    for s, r in enumerate(rows):
        out = jnp.where(ids == s, r, out)
    return out


def centre(shape):
    parts = [lax.axis_index(ax).astype(F32) * SIDE + 0.5 * SIDE for ax in AXES]
    return pick_rows(parts, shape)


def scaled(x, mid, unit):
    n = x.shape[1]
    full = jnp.concatenate([x[:3], jnp.zeros((5, n), F32)], axis=0)
    return (full - mid) * (1.0 / unit)


def receiver_matrix(u):
    h, m, l = split3(u)
    norm = 1.0 - jnp.sum(u * u, axis=0, keepdims=True)
    a, b, c = split3(norm)
    h, m, l = 2.0 * h, 2.0 * m, 2.0 * l
    one = jnp.ones_like(norm)
    tail = pick_rows([a, b, c, one, one, one], u.shape)
    return jnp.concatenate([h, h, h, m, m, l, tail, jnp.zeros_like(u)], axis=0).astype(BF16)


def source_matrices(u, valid=None):
    h, m, l = split3(u)
    norm = -jnp.sum(u * u, axis=0, keepdims=True)
    if valid is not None:
        norm = jnp.where(valid, norm, FAR)
    a, b, c = split3(norm)
    one = jnp.ones_like(norm)
    tail = pick_rows([one, one, one, a, b, c], u.shape)
    pair = jnp.concatenate([h, m, l, h, m, h, tail, jnp.zeros_like(u)], axis=0)
    ids = row_ids(u.shape)
    total = jnp.concatenate([jnp.where(ids == 3, 1.0, h), m, l], axis=0)
    return pair, total


def dot(a, b):
    return jnp.dot(a, b, preferred_element_type=F32)


def two_parts(w):
    return w, w - rounded(w)


def gather_lanes(sources, index):
    index = jnp.broadcast_to(index, (8, LANES))
    tile = lax.shift_right_logical(index, 7)
    lane = lax.bitwise_and(index, LANES - 1)
    out = jnp.zeros((8, LANES), F32)
    for r, src in enumerate(sources):
        out = jnp.where(tile == r, jnp.take_along_axis(src, lane, axis=1), out)
    return out


def lane_tiles(a):
    return [a[:, r * LANES : (r + 1) * LANES] for r in range(a.shape[1] // LANES)]


def pad8(x):
    return jnp.concatenate([x, jnp.zeros((8 - x.shape[0], x.shape[1]), F32)], axis=0)


def write_faces(swaps, x, charge, index_ref, send_refs):
    rows = [x] if charge is None else [x, charge]
    tiles = lane_tiles(pad8(jnp.concatenate(rows, axis=0)))
    for (axis, phase, _), ref in zip(swaps, send_refs):
        even = lax.axis_index(AXES[axis]) % 2 == 0
        high = even if phase == 0 else jnp.logical_not(even)
        index = jnp.where(high, index_ref[2 * axis + 1 : 2 * axis + 2, :], index_ref[2 * axis : 2 * axis + 1, :])
        for w in range(index.shape[1] // LANES):
            part = slice(w * LANES, (w + 1) * LANES)
            ref[:, part] = gather_lanes(tiles, index[:, part])[:4]


def start_kernel(swaps, *refs):
    sources, refs = refs[:N_START], refs[N_START:]
    x_ref, mass_ref, index_ref = refs[:3]
    kept, refs = refs[3 : N_START - 3], refs[N_START - 3 :]
    x_out, v_out = refs[:2]
    send_refs, (v_ref, fast_ref, slow_ref, sems) = refs[2 : 2 + len(swaps)], refs[2 + len(swaps) :]
    kept = [x_ref, mass_ref, index_ref, v_ref, fast_ref, slow_ref, *kept]
    copies = [
        pltpu.make_async_copy(src, dst, sems.at[k]) for k, (src, dst) in enumerate(zip(sources, kept))
    ]
    for c in copies:
        c.start()
    for c in copies[:6]:
        c.wait()
    mass = mass_ref[...]
    v = v_ref[...] + (0.5 * INNER * STEP) * mass * slow_ref[...]
    v = v + (0.5 * STEP) * mass * fast_ref[...]
    x = x_ref[...] + STEP * v
    x_out[...] = x
    v_out[...] = v
    write_faces(swaps, x, None, index_ref, send_refs)
    for c in copies[6:]:
        c.wait()


def pair_sums(receivers, sources, totals, fold=None):
    sums = []
    for it in range(len(receivers)):
        out = None
        for st in range(len(sources)):
            closeness = dot(sources[st], receivers[it])
            high, low = two_parts(jnp.maximum(closeness, 0.0))
            part = dot(totals[st], high) + dot(totals[st], low)
            if fold is not None:
                part = fold(it, st, part)
            out = part if out is None else out + part
        sums.append(out)
    return sums


def short_from(u, sums):
    part = sums[0:8] + sums[8:16] + sums[16:24]
    return SHORT_UNIT * (u * part[3:4] - part)


def blocks(a, width=BLOCK):
    return [a[:, s : s + width] for s in range(0, a.shape[1], width)]


def tile_counts(own_ref, partner_ref, count_ref, n_tiles, swaps):
    slots = own_ref.shape[1]
    partner = partner_ref[...]
    own = own_ref[...]
    live = lax.broadcasted_iota(jnp.int32, (1, slots), 1) < count_ref[...]
    outside = partner - n_tiles
    axis = lax.shift_right_logical(outside, 2)
    side = lax.bitwise_and(lax.shift_right_logical(outside, 1), 1)
    within = lax.bitwise_and(outside, 1)
    place = jnp.full_like(partner, -1)
    for k, (ax, phase, _) in enumerate(swaps):
        even = lax.axis_index(AXES[ax]) % 2 == 0
        high = even if phase == 0 else jnp.logical_not(even)
        want = jnp.where(high, 1, 0)
        place = jnp.where((axis == ax) & (side == want), n_tiles + 2 * k + within, place)
    place = jnp.where(outside < 0, partner, place)
    own_hot = jnp.where((row_ids((8, slots)) == own) & live, 1.0, 0.0)
    place_hot = jnp.where(row_ids((32, slots)) == place, 1.0, 0.0)
    return lax.dot_general(own_hot, place_hot, (((1,), (1,)), ((), ())), preferred_element_type=F32)


def slow_totals(u, charge):
    base = jnp.where(row_ids(u.shape) == 3, 1.0, u) * charge
    rows = jnp.concatenate(split3(base), axis=0)
    first = lax.broadcasted_iota(jnp.int32, rows.shape, 1) < LANES
    return jnp.concatenate([jnp.where(first, rows, 0.0), jnp.where(first, 0.0, rows)], axis=0)


def slow_fold(counts, first_tile):
    wide = {}

    def row(it, u):
        if u not in wide:
            wide[u] = jnp.broadcast_to(counts[:, u : u + 1], (8, LANES))
        return jnp.concatenate([wide[u][2 * it : 2 * it + 1], wide[u][2 * it + 1 : 2 * it + 2]], axis=1)

    def fold(it, st, part):
        u = first_tile + 2 * st
        return part[:24] * row(it, u) + part[24:] * row(it, u + 1)

    return fold


def slow_from(u, charge, sums):
    part = sums[0:8] + sums[8:16] + sums[16:24]
    return (LONG_SCALE * LONG_UNIT) * charge * (u * part[3:4] - part)


def slow_own_kernel(swaps, x_ref, charge_ref, own_ref, partner_ref, count_ref, slow_out, counts_out):
    n = x_ref.shape[1]
    charge = charge_ref[...]
    u = scaled(x_ref[...], centre((8, n)), LONG_UNIT)
    pair, _ = source_matrices(u)
    counts = tile_counts(own_ref, partner_ref, count_ref, n // LANES, swaps)
    counts_out[...] = counts
    sums = pair_sums(
        blocks(receiver_matrix(u)),
        [jnp.transpose(p).astype(BF16) for p in blocks(pair)],
        [slow_totals(b, q) for b, q in zip(blocks(u), blocks(charge))],
        slow_fold(counts, 0),
    )
    slow_out[...] = slow_from(u, charge, jnp.concatenate(sums, axis=1))[:3]


def slow_halo_kernel(swaps, *refs):
    x_ref, v_ref, mass_ref, charge_ref, counts_ref, slow_ref, force_ref, start_ref = refs[:8]
    arrived, refs = refs[8 : 8 + len(swaps)], refs[8 + len(swaps) :]
    outs, (moved, v_new, slow_new, sems) = refs[:4], refs[4:]
    x = x_ref[...]
    n = x.shape[1]
    moved[...] = x - start_ref[...]
    copies = [
        pltpu.make_async_copy(src, dst, sems.at[k])
        for k, (src, dst) in enumerate(zip([moved, v_new, force_ref, slow_new], outs))
    ]
    copies[0].start()
    copies[2].start()
    u = scaled(x, centre((8, n)), LONG_UNIT)
    charge = charge_ref[...]
    sources, totals = [], []
    for swap, ref in zip(swaps, arrived):
        got = ref[...]
        there, valid = halo_place(swap, got, LONG_UNIT)
        sources.append(jnp.transpose(source_matrices(there, valid)[0]).astype(BF16))
        totals.append(slow_totals(there, got[3:4]))
    sums = pair_sums(
        blocks(receiver_matrix(u)), sources, totals, slow_fold(counts_ref[...], n // LANES)
    )
    slow = slow_ref[...] + slow_from(u, charge, jnp.concatenate(sums, axis=1))[:3]
    slow_new[...] = slow
    v_new[...] = v_ref[...] + (0.5 * INNER * STEP) * mass_ref[...] * slow
    copies[1].start()
    copies[3].start()
    for c in copies:
        c.wait()


def halo_place(swap, got, unit):
    axis, phase, _ = swap
    place = lax.axis_index(AXES[axis])
    valid = place >= 0
    if phase:
        valid = (place > 0) & (place < lax.axis_size(AXES[axis]) - 1)
    there = scaled(got, centre((8, got.shape[1])), unit)
    return jnp.where(valid, there, 0.0), valid


def own_kernel(first, *refs):
    x_ref, bonds_ref, bond_k_ref = refs[:3]
    out_ref, incidence = refs[3:] if first else (refs[4], refs[3])
    x = x_ref[...]
    n = x.shape[1]
    tiles = lane_tiles(pad8(x))
    pulls = []
    for t in range(n // LANES):
        part = slice(t * LANES, (t + 1) * LANES)
        gap = gather_lanes(tiles, bonds_ref[0:1, part]) - gather_lanes(tiles, bonds_ref[1:2, part])
        pulls.append(bond_k_ref[:, part] * gap)
    pull = jnp.concatenate(pulls, axis=1)
    pull = jnp.concatenate(split3(pull), axis=0).astype(BF16)
    if first:
        for t in range(n // LANES):
            part = slice(t * LANES, (t + 1) * LANES)
            i = jnp.transpose(jnp.broadcast_to(bonds_ref[0:1, part], (LANES, LANES)))
            j = jnp.transpose(jnp.broadcast_to(bonds_ref[1:2, part], (LANES, LANES)))
            for s in range(n // LANES):
                atom = lax.broadcasted_iota(jnp.int32, (LANES, LANES), 1) + s * LANES
                hit = jnp.where(j == atom, 1.0, 0.0)
                hit = jnp.where(i == atom, hit - 1.0, hit)
                incidence[part, s * LANES : (s + 1) * LANES] = hit.astype(BF16)
    bonded = dot(pull, incidence[...])
    bonded = bonded[0:8] + bonded[8:16] + bonded[16:24]

    u = scaled(x, centre((8, n)), SHORT_UNIT)
    pair, total = source_matrices(u)
    sums = pair_sums(
        blocks(receiver_matrix(u)),
        [jnp.transpose(p).astype(BF16) for p in blocks(pair)],
        blocks(total),
    )
    force = short_from(u, jnp.concatenate(sums, axis=1)) + bonded
    out_ref[...] = force[:3]


def halo_kernel(swaps, last, send_charge, *refs):
    x_ref, v_ref, mass_ref, force_ref = refs[:4]
    arrived, refs = refs[4 : 4 + len(swaps)], refs[4 + len(swaps) :]
    x = x_ref[...]
    u = scaled(x, centre((8, x.shape[1])), SHORT_UNIT)
    sources, totals = [], []
    for swap, ref in zip(swaps, arrived):
        pair, total = source_matrices(*halo_place(swap, ref[...], SHORT_UNIT))
        sources.append(jnp.transpose(pair).astype(BF16))
        totals.append(total)
    sums = pair_sums(blocks(receiver_matrix(u)), sources, totals)
    mass = mass_ref[...]
    force = force_ref[...] + short_from(u, jnp.concatenate(sums, axis=1))[:3]
    v = v_ref[...] + (0.5 * STEP) * mass * force
    if last:
        force_out, v_out = refs
        force_out[...] = force
        v_out[...] = v
        return
    index_ref, refs = refs[0], refs[1:]
    charge = None
    if send_charge:
        charge, refs = refs[0][...], refs[1:]
    v = v + (0.5 * STEP) * mass * force
    x = x + STEP * v
    refs[0][...] = x
    refs[1][...] = v
    write_faces(swaps, x, charge, index_ref, refs[2:])


def call(kernel, outs, args, flops=0):
    return pl.pallas_call(
        kernel,
        out_shape=[jax.ShapeDtypeStruct(s, d) for s, d in outs],
        in_specs=[pl.BlockSpec(memory_space=pltpu.VMEM)] * len(args),
        out_specs=[pl.BlockSpec(memory_space=pltpu.VMEM)] * len(outs),
        compiler_params=pltpu.CompilerParams(vmem_limit_bytes=24 * 1024 * 1024),
        cost_estimate=pl.CostEstimate(flops=flops, bytes_accessed=100000, transcendentals=0),
    )(*args)


def on_device(
    swaps,
    positions,
    velocities,
    inv_mass,
    charge,
    fast_force,
    slow_force,
    bonds,
    bond_k,
    halo_index,
    pair_own,
    pair_partner,
    pair_count,
):
    n = positions.shape[1]
    vec = ((3, n), F32)
    sends = [((4, halo_index.shape[1]), F32)] * len(swaps)
    start_args = [positions, inv_mass.reshape(1, n), halo_index, velocities, fast_force, slow_force]
    start_args += [charge.reshape(1, n), bonds, bond_k.reshape(1, -1)]
    start_args += [pair_own.reshape(1, -1), pair_partner.reshape(1, -1), pair_count.reshape(1, 1)]
    assert len(start_args) == N_START
    kept = [(a.shape, a.dtype) for a in start_args[:3] + start_args[6:]]
    start_args = [pltpu.with_memory_space_constraint(a, pltpu.HBM) for a in start_args[:-1]] + start_args[-1:]
    start, mass, index, charge, bonds, bond_k, own, partner, count, x, v, *faces = pl.pallas_call(
        functools.partial(start_kernel, swaps),
        out_shape=[jax.ShapeDtypeStruct(s, d) for s, d in kept + [vec, vec] + sends],
        in_specs=[pl.BlockSpec(memory_space=pltpu.HBM)] * N_START,
        out_specs=[pl.BlockSpec(memory_space=pltpu.VMEM)] * (len(kept) + 2 + len(sends)),
        scratch_shapes=[pltpu.VMEM((3, n), F32)] * 3 + [pltpu.SemaphoreType.DMA((N_START,))],
        compiler_params=pltpu.CompilerParams(vmem_limit_bytes=4 * 1024 * 1024),
    )(*start_args)
    incidence = None
    for turn in range(INNER):
        first, last = turn == 0, turn == INNER - 1
        arrived = [lax.ppermute(f, AXES, perm) for f, (_, _, perm) in zip(faces, swaps)]
        outs, args = [vec], [x, bonds, bond_k]
        if first:
            outs.append(((bonds.shape[1], n), BF16))
        else:
            args.append(incidence)
        force, *built = call(functools.partial(own_kernel, first), outs, args, flops=2 * 10**9)
        if first:
            incidence = built[0]
        args = [x, v, mass, force] + arrived
        if last:
            slow, counts = call(
                functools.partial(slow_own_kernel, swaps),
                [vec, ((8, 32), F32)],
                [x, charge, own, partner, count],
                flops=2 * 10**9,
            )
            force, v = call(
                functools.partial(halo_kernel, swaps, True, False), [vec, vec], args, flops=10**9
            )
            break
        args.append(index)
        send_charge = turn == INNER - 2
        if send_charge:
            args.append(charge)
        x, v, *faces = call(
            functools.partial(halo_kernel, swaps, False, send_charge),
            [vec, vec] + sends,
            args,
            flops=10**9,
        )
    args = [x, v, mass, charge, counts, slow, force, start] + arrived
    return pl.pallas_call(
        functools.partial(slow_halo_kernel, swaps),
        out_shape=[jax.ShapeDtypeStruct(*vec)] * 4,
        in_specs=[pl.BlockSpec(memory_space=pltpu.VMEM)] * len(args),
        out_specs=[pl.BlockSpec(memory_space=pltpu.HBM)] * 4,
        scratch_shapes=[pltpu.VMEM((3, n), F32)] * 3 + [pltpu.SemaphoreType.DMA((4,))],
        compiler_params=pltpu.CompilerParams(vmem_limit_bytes=24 * 1024 * 1024),
    )(*args)


def solution(mesh):
    rows = P(None, AXES)
    flat = P(AXES)
    swaps = matchings([mesh.shape[ax] for ax in AXES])
    return jax.shard_map(
        functools.partial(on_device, swaps),
        mesh=mesh,
        in_specs=(rows, rows, flat, flat, rows, rows, rows, flat, rows, flat, flat, flat),
        out_specs=(rows, rows, rows, rows),
        check_vma=False,
    )
```

```python
import functools

import jax
import jax.numpy as jnp
from jax import lax
from jax.experimental import pallas as pl
from jax.experimental.pallas import tpu as pltpu
from jax.sharding import PartitionSpec as P

AXES = ("gx", "gy", "gz")
INNER = 4
STEP = 0.1
LONG_SCALE = 0.5
SIDE = 4.0
SHORT_UNIT = 0.8
LONG_UNIT = 1.2
LANES = 128
BLOCK = 256
FAR = -1.0e6

N_START = 12
F32 = jnp.float32
BF16 = jnp.bfloat16


def matchings(sizes):
    nx, ny, nz = sizes
    assert nx % 2 == 0 and ny % 2 == 0 and nz % 2 == 0
    swaps = []
    for axis, phase in ((2, 0), (2, 1), (1, 1), (0, 0), (0, 1), (1, 0)):
        if phase and sizes[axis] == 2:
            continue
        perm = []
        for a in range(nx):
            for b in range(ny):
                for c in range(nz):
                    place = [a, b, c]
                    p = place[axis]
                    partner = p ^ 1 if phase == 0 else (p + 1 if p % 2 else p - 1)
                    if 0 <= partner < sizes[axis]:
                        place[axis] = partner
                    elif axis == 1:
                        place[1] = ny - 1 - p
                    else:
                        place[1] ^= 1
                    source = (a * ny + b) * nz + c
                    perm.append((source, (place[0] * ny + place[1]) * nz + place[2]))
        swaps.append((axis, phase, perm))
    return swaps


def rounded(a):
    return a.astype(BF16).astype(F32)


def split3(a):
    high = rounded(a)
    rest = a - high
    mid = rounded(rest)
    return high, mid, rounded(rest - mid)


def row_ids(shape):
    return lax.broadcasted_iota(jnp.int32, shape, 0)


def pick_rows(rows, shape):
    ids = row_ids(shape)
    out = jnp.zeros(shape, F32)
    for s, r in enumerate(rows):
        out = jnp.where(ids == s, r, out)
    return out


def centre(shape):
    parts = [lax.axis_index(ax).astype(F32) * SIDE + 0.5 * SIDE for ax in AXES]
    return pick_rows(parts, shape)


def scaled(x, mid, unit):
    n = x.shape[1]
    full = jnp.concatenate([x[:3], jnp.zeros((5, n), F32)], axis=0)
    return (full - mid) * (1.0 / unit)


def receiver_matrix(u):
    h, m, l = split3(u)
    norm = 1.0 - jnp.sum(u * u, axis=0, keepdims=True)
    a, b, c = split3(norm)
    h, m, l = 2.0 * h, 2.0 * m, 2.0 * l
    one = jnp.ones_like(norm)
    tail = pick_rows([a, b, c, one, one, one], u.shape)
    return jnp.concatenate([h, h, h, m, m, l, tail, jnp.zeros_like(u)], axis=0).astype(BF16)


def source_matrices(u, valid=None):
    h, m, l = split3(u)
    norm = -jnp.sum(u * u, axis=0, keepdims=True)
    if valid is not None:
        norm = jnp.where(valid, norm, FAR)
    a, b, c = split3(norm)
    one = jnp.ones_like(norm)
    tail = pick_rows([one, one, one, a, b, c], u.shape)
    pair = jnp.concatenate([h, m, l, h, m, h, tail, jnp.zeros_like(u)], axis=0)
    ids = row_ids(u.shape)
    total = jnp.concatenate([jnp.where(ids == 3, 1.0, h), m, l], axis=0)
    return pair, total


def dot(a, b):
    return jnp.dot(a, b, preferred_element_type=F32)


def two_parts(w):
    return w, w - rounded(w)


def pad8(x):
    return jnp.concatenate([x, jnp.zeros((8 - x.shape[0], x.shape[1]), F32)], axis=0)


def gather_grid(x, index):
    tile = lax.shift_right_logical(index, 7)
    lane = lax.bitwise_and(index, LANES - 1)
    hits = [tile == r for r in range(1, x.shape[1] // LANES)]
    out = []
    for c in range(x.shape[0]):
        got = None
        for r in range(x.shape[1] // LANES):
            row = jnp.broadcast_to(x[c : c + 1, r * LANES : (r + 1) * LANES], (8, LANES))
            here = jnp.take_along_axis(row, lane, axis=1)
            got = here if got is None else jnp.where(hits[r - 1], here, got)
        out.append(got)
    return out


def write_faces(x, index_ref, send_refs):
    per = send_refs[0].shape[1] // LANES
    for g in range(index_ref.shape[0] // 8):
        got = gather_grid(x, index_ref[8 * g : 8 * g + 8, :])
        for r in range(8 * g, min(8 * g + 8, per * len(send_refs))):
            part = slice(r % per * LANES, (r % per + 1) * LANES)
            for c, rows in enumerate(got):
                send_refs[r // per][c : c + 1, part] = rows[r % 8 : r % 8 + 1]


def write_face_index(swaps, index_ref, out_ref):
    per = index_ref.shape[1] // LANES
    out_ref[...] = jnp.zeros_like(out_ref)
    for k, (axis, phase, _) in enumerate(swaps):
        even = lax.axis_index(AXES[axis]) % 2 == 0
        high = even if phase == 0 else jnp.logical_not(even)
        low_row, high_row = index_ref[2 * axis : 2 * axis + 1, :], index_ref[2 * axis + 1 : 2 * axis + 2, :]
        row = jnp.where(high, high_row, low_row)
        for w in range(per):
            out_ref[per * k + w : per * k + w + 1, :] = row[:, w * LANES : (w + 1) * LANES]


def write_grid(row_ref, out_ref):
    for t in range(out_ref.shape[1]):
        for e in range(out_ref.shape[0]):
            out_ref[e, t : t + 1, :] = row_ref[e : e + 1, t * LANES : (t + 1) * LANES]


def start_kernel(swaps, *refs):
    sources, refs = refs[:N_START], refs[N_START:]
    x_ref, mass_ref, charge_ref, own_ref, partner_ref, count_ref = refs[:6]
    index_out, bonds_out, bond_k_out, x_out, v_out = refs[6:11]
    send_refs, refs = refs[11 : 11 + len(swaps)], refs[11 + len(swaps) :]
    v_ref, fast_ref, slow_ref, index_ref, bonds_ref, bond_k_ref, sems = refs
    kept = [x_ref, mass_ref, index_ref, v_ref, fast_ref, slow_ref]
    kept += [charge_ref, bonds_ref, bond_k_ref, own_ref, partner_ref, count_ref]
    copies = [
        pltpu.make_async_copy(src, dst, sems.at[k]) for k, (src, dst) in enumerate(zip(sources, kept))
    ]
    for c in copies:
        c.start()
    for c in copies[:6]:
        c.wait()
    write_face_index(swaps, index_ref, index_out)
    mass = mass_ref[...]
    v = v_ref[...] + (0.5 * INNER * STEP) * mass * slow_ref[...]
    v = v + (0.5 * STEP) * mass * fast_ref[...]
    x = x_ref[...] + STEP * v
    x_out[...] = x
    v_out[...] = v
    write_faces(x, index_out, send_refs)
    for c in copies[6:]:
        c.wait()
    write_grid(bonds_ref, bonds_out)
    write_grid(bond_k_ref, bond_k_out)


def pair_sums(receivers, sources, totals, fold=None):
    sums = []
    for it in range(len(receivers)):
        out = None
        for st in range(len(sources)):
            closeness = dot(sources[st], receivers[it])
            high, low = two_parts(jnp.maximum(closeness, 0.0))
            part = dot(totals[st], high) + dot(totals[st], low)
            if fold is not None:
                part = fold(it, st, part)
            out = part if out is None else out + part
        sums.append(out)
    return sums


def short_from(u, sums):
    part = sums[0:8] + sums[8:16] + sums[16:24]
    return SHORT_UNIT * (u * part[3:4] - part)


def blocks(a, width=BLOCK):
    return [a[:, s : s + width] for s in range(0, a.shape[1], width)]


def tile_counts(own_ref, partner_ref, count_ref, n_tiles, swaps):
    slots = own_ref.shape[1]
    partner = partner_ref[...]
    own = own_ref[...]
    live = lax.broadcasted_iota(jnp.int32, (1, slots), 1) < count_ref[...]
    outside = partner - n_tiles
    axis = lax.shift_right_logical(outside, 2)
    side = lax.bitwise_and(lax.shift_right_logical(outside, 1), 1)
    within = lax.bitwise_and(outside, 1)
    place = jnp.full_like(partner, -1)
    for k, (ax, phase, _) in enumerate(swaps):
        even = lax.axis_index(AXES[ax]) % 2 == 0
        high = even if phase == 0 else jnp.logical_not(even)
        want = jnp.where(high, 1, 0)
        place = jnp.where((axis == ax) & (side == want), n_tiles + 2 * k + within, place)
    place = jnp.where(outside < 0, partner, place)
    own_hot = jnp.where((row_ids((8, slots)) == own) & live, 1.0, 0.0)
    place_hot = jnp.where(row_ids((32, slots)) == place, 1.0, 0.0)
    return lax.dot_general(own_hot, place_hot, (((1,), (1,)), ((), ())), preferred_element_type=F32)


def slow_totals(u, charge):
    base = jnp.where(row_ids(u.shape) == 3, 1.0, u) * charge
    rows = jnp.concatenate(split3(base), axis=0)
    first = lax.broadcasted_iota(jnp.int32, rows.shape, 1) < LANES
    return jnp.concatenate([jnp.where(first, rows, 0.0), jnp.where(first, 0.0, rows)], axis=0)


def slow_fold(counts, first_tile):
    wide = {}

    def row(it, u):
        if u not in wide:
            wide[u] = jnp.broadcast_to(counts[:, u : u + 1], (8, LANES))
        return jnp.concatenate([wide[u][2 * it : 2 * it + 1], wide[u][2 * it + 1 : 2 * it + 2]], axis=1)

    def fold(it, st, part):
        u = first_tile + 2 * st
        return part[:24] * row(it, u) + part[24:] * row(it, u + 1)

    return fold


def slow_from(u, charge, sums):
    part = sums[0:8] + sums[8:16] + sums[16:24]
    return (LONG_SCALE * LONG_UNIT) * charge * (u * part[3:4] - part)


def slow_own_kernel(swaps, x_ref, charge_ref, own_ref, partner_ref, count_ref, slow_out, counts_out):
    n = x_ref.shape[1]
    charge = charge_ref[...]
    u = scaled(x_ref[...], centre((8, n)), LONG_UNIT)
    pair, _ = source_matrices(u)
    counts = tile_counts(own_ref, partner_ref, count_ref, n // LANES, swaps)
    counts_out[...] = counts
    sums = pair_sums(
        blocks(receiver_matrix(u)),
        [jnp.transpose(p).astype(BF16) for p in blocks(pair)],
        [slow_totals(b, q) for b, q in zip(blocks(u), blocks(charge))],
        slow_fold(counts, 0),
    )
    slow_out[...] = slow_from(u, charge, jnp.concatenate(sums, axis=1))[:3]


def slow_halo_kernel(swaps, *refs):
    x_ref, v_ref, mass_ref, charge_ref, counts_ref, slow_ref, force_ref, start_ref = refs[:8]
    arrived, refs = refs[8 : 8 + len(swaps)], refs[8 + len(swaps) :]
    outs, (moved, v_new, slow_new, sems) = refs[:4], refs[4:]
    x = x_ref[...]
    n = x.shape[1]
    moved[...] = x - start_ref[...]
    copies = [
        pltpu.make_async_copy(src, dst, sems.at[k])
        for k, (src, dst) in enumerate(zip([moved, v_new, force_ref, slow_new], outs))
    ]
    copies[0].start()
    copies[2].start()
    u = scaled(x, centre((8, n)), LONG_UNIT)
    charge = charge_ref[...]
    sources, totals = [], []
    for swap, ref in zip(swaps, arrived):
        got = ref[...]
        there, valid = halo_place(swap, got, LONG_UNIT)
        sources.append(jnp.transpose(source_matrices(there, valid)[0]).astype(BF16))
        totals.append(slow_totals(there, got[3:4]))
    sums = pair_sums(
        blocks(receiver_matrix(u)), sources, totals, slow_fold(counts_ref[...], n // LANES)
    )
    slow = slow_ref[...] + slow_from(u, charge, jnp.concatenate(sums, axis=1))[:3]
    slow_new[...] = slow
    v_new[...] = v_ref[...] + (0.5 * INNER * STEP) * mass_ref[...] * slow
    copies[1].start()
    copies[3].start()
    for c in copies:
        c.wait()


def halo_place(swap, got, unit):
    axis, phase, _ = swap
    place = lax.axis_index(AXES[axis])
    valid = place >= 0
    if phase:
        valid = (place > 0) & (place < lax.axis_size(AXES[axis]) - 1)
    there = scaled(got, centre((8, got.shape[1])), unit)
    return jnp.where(valid, there, 0.0), valid


def own_kernel(first, *refs):
    x_ref, bonds_ref, bond_k_ref = refs[:3]
    out_ref, incidence = refs[3:] if first else (refs[4], refs[3])
    x = x_ref[...]
    n = x.shape[1]
    pulls = []
    for g in range(bonds_ref.shape[1] // 8):
        rows = slice(8 * g, 8 * g + 8)
        ends = zip(gather_grid(x, bonds_ref[0, rows, :]), gather_grid(x, bonds_ref[1, rows, :]))
        pull = [bond_k_ref[0, rows, :] * (i - j) for i, j in ends]
        for t in range(8):
            pulls.append(jnp.concatenate([p[t : t + 1] for p in pull], axis=0))
    pull = pad8(jnp.concatenate(pulls, axis=1))
    pull = jnp.concatenate(split3(pull), axis=0).astype(BF16)
    if first:
        for t in range(bonds_ref.shape[1]):
            part = slice(t * LANES, (t + 1) * LANES)
            i = jnp.transpose(jnp.broadcast_to(bonds_ref[0, t : t + 1, :], (LANES, LANES)))
            j = jnp.transpose(jnp.broadcast_to(bonds_ref[1, t : t + 1, :], (LANES, LANES)))
            for s in range(n // LANES):
                atom = lax.broadcasted_iota(jnp.int32, (LANES, LANES), 1) + s * LANES
                hit = jnp.where(j == atom, 1.0, 0.0)
                hit = jnp.where(i == atom, hit - 1.0, hit)
                incidence[part, s * LANES : (s + 1) * LANES] = hit.astype(BF16)
    bonded = dot(pull, incidence[...])
    bonded = bonded[0:8] + bonded[8:16] + bonded[16:24]

    u = scaled(x, centre((8, n)), SHORT_UNIT)
    pair, total = source_matrices(u)
    sums = pair_sums(
        blocks(receiver_matrix(u)),
        [jnp.transpose(p).astype(BF16) for p in blocks(pair)],
        blocks(total),
    )
    force = short_from(u, jnp.concatenate(sums, axis=1)) + bonded
    out_ref[...] = force[:3]


def halo_kernel(swaps, last, send_charge, *refs):
    x_ref, v_ref, mass_ref, force_ref = refs[:4]
    arrived, refs = refs[4 : 4 + len(swaps)], refs[4 + len(swaps) :]
    x = x_ref[...]
    u = scaled(x, centre((8, x.shape[1])), SHORT_UNIT)
    sources, totals = [], []
    for swap, ref in zip(swaps, arrived):
        pair, total = source_matrices(*halo_place(swap, ref[...], SHORT_UNIT))
        sources.append(jnp.transpose(pair).astype(BF16))
        totals.append(total)
    sums = pair_sums(blocks(receiver_matrix(u)), sources, totals)
    mass = mass_ref[...]
    force = force_ref[...] + short_from(u, jnp.concatenate(sums, axis=1))[:3]
    v = v_ref[...] + (0.5 * STEP) * mass * force
    if last:
        force_out, v_out = refs
        force_out[...] = force
        v_out[...] = v
        return
    index_ref, refs = refs[0], refs[1:]
    charge = None
    if send_charge:
        charge, refs = refs[0][...], refs[1:]
    v = v + (0.5 * STEP) * mass * force
    x = x + STEP * v
    refs[0][...] = x
    refs[1][...] = v
    if send_charge:
        x = jnp.concatenate([x, charge], axis=0)
    write_faces(x, index_ref, refs[2:])


def call(kernel, outs, args, flops=0):
    return pl.pallas_call(
        kernel,
        out_shape=[jax.ShapeDtypeStruct(s, d) for s, d in outs],
        in_specs=[pl.BlockSpec(memory_space=pltpu.VMEM)] * len(args),
        out_specs=[pl.BlockSpec(memory_space=pltpu.VMEM)] * len(outs),
        compiler_params=pltpu.CompilerParams(vmem_limit_bytes=24 * 1024 * 1024),
        cost_estimate=pl.CostEstimate(flops=flops, bytes_accessed=100000, transcendentals=0),
    )(*args)


def on_device(
    swaps,
    positions,
    velocities,
    inv_mass,
    charge,
    fast_force,
    slow_force,
    bonds,
    bond_k,
    halo_index,
    pair_own,
    pair_partner,
    pair_count,
):
    n = positions.shape[1]
    vec = ((3, n), F32)
    sends = [((4, halo_index.shape[1]), F32)] * len(swaps)
    start_args = [positions, inv_mass.reshape(1, n), halo_index, velocities, fast_force, slow_force]
    start_args += [charge.reshape(1, n), bonds, bond_k.reshape(1, -1)]
    start_args += [pair_own.reshape(1, -1), pair_partner.reshape(1, -1), pair_count.reshape(1, 1)]
    assert len(start_args) == N_START
    kept = [(start_args[k].shape, start_args[k].dtype) for k in (0, 1, 6, 9, 10, 11)]
    n_bonds = bonds.shape[1]
    face_rows = len(swaps) * halo_index.shape[1] // LANES
    kept.append(((-(-face_rows // 8) * 8, LANES), jnp.int32))
    kept.append(((2, n_bonds // LANES, LANES), jnp.int32))
    kept.append(((1, n_bonds // LANES, LANES), F32))
    scratch = [pltpu.VMEM((3, n), F32)] * 3
    scratch += [pltpu.VMEM(halo_index.shape, jnp.int32), pltpu.VMEM(bonds.shape, jnp.int32)]
    scratch += [pltpu.VMEM((1, n_bonds), F32), pltpu.SemaphoreType.DMA((N_START,))]
    start_args = [pltpu.with_memory_space_constraint(a, pltpu.HBM) for a in start_args[:-1]] + start_args[-1:]
    start, mass, charge, own, partner, count, index, bonds, bond_k, x, v, *faces = pl.pallas_call(
        functools.partial(start_kernel, swaps),
        out_shape=[jax.ShapeDtypeStruct(s, d) for s, d in kept + [vec, vec] + sends],
        in_specs=[pl.BlockSpec(memory_space=pltpu.HBM)] * N_START,
        out_specs=[pl.BlockSpec(memory_space=pltpu.VMEM)] * (len(kept) + 2 + len(sends)),
        scratch_shapes=scratch,
        compiler_params=pltpu.CompilerParams(vmem_limit_bytes=4 * 1024 * 1024),
    )(*start_args)
    incidence = None
    for turn in range(INNER):
        first, last = turn == 0, turn == INNER - 1
        arrived = [lax.ppermute(f, AXES, perm) for f, (_, _, perm) in zip(faces, swaps)]
        outs, args = [vec], [x, bonds, bond_k]
        if first:
            outs.append(((n_bonds, n), BF16))
        else:
            args.append(incidence)
        force, *built = call(functools.partial(own_kernel, first), outs, args, flops=2 * 10**9)
        if first:
            incidence = built[0]
        args = [x, v, mass, force] + arrived
        if last:
            slow, counts = call(
                functools.partial(slow_own_kernel, swaps),
                [vec, ((8, 32), F32)],
                [x, charge, own, partner, count],
                flops=2 * 10**9,
            )
            force, v = call(
                functools.partial(halo_kernel, swaps, True, False), [vec, vec], args, flops=10**9
            )
            break
        args.append(index)
        send_charge = turn == INNER - 2
        if send_charge:
            args.append(charge)
        x, v, *faces = call(
            functools.partial(halo_kernel, swaps, False, send_charge),
            [vec, vec] + sends,
            args,
            flops=10**9,
        )
    args = [x, v, mass, charge, counts, slow, force, start] + arrived
    return pl.pallas_call(
        functools.partial(slow_halo_kernel, swaps),
        out_shape=[jax.ShapeDtypeStruct(*vec)] * 4,
        in_specs=[pl.BlockSpec(memory_space=pltpu.VMEM)] * len(args),
        out_specs=[pl.BlockSpec(memory_space=pltpu.HBM)] * 4,
        scratch_shapes=[pltpu.VMEM((3, n), F32)] * 3 + [pltpu.SemaphoreType.DMA((4,))],
        compiler_params=pltpu.CompilerParams(vmem_limit_bytes=24 * 1024 * 1024),
    )(*args)


def solution(mesh):
    rows = P(None, AXES)
    flat = P(AXES)
    swaps = matchings([mesh.shape[ax] for ax in AXES])
    return jax.shard_map(
        functools.partial(on_device, swaps),
        mesh=mesh,
        in_specs=(rows, rows, flat, flat, rows, rows, rows, flat, rows, flat, flat, flat),
        out_specs=(rows, rows, rows, rows),
        check_vma=False,
    )
```

```python
import functools

import jax
import jax.numpy as jnp
from jax import lax
from jax.experimental import pallas as pl
from jax.experimental.pallas import tpu as pltpu
from jax.sharding import PartitionSpec as P

AXES = ("gx", "gy", "gz")
INNER = 4
STEP = 0.1
LONG_SCALE = 0.5
SIDE = 4.0
SHORT_UNIT = 0.8
LONG_UNIT = 1.2
LANES = 128
BLOCK = 256
FAR = -1.0e6

N_START = 10
F32 = jnp.float32
BF16 = jnp.bfloat16


def matchings(sizes):
    nx, ny, nz = sizes
    assert nx % 2 == 0 and ny % 2 == 0 and nz % 2 == 0
    swaps = []
    for axis, phase in ((2, 0), (2, 1), (1, 1), (0, 0), (0, 1), (1, 0)):
        if phase and sizes[axis] == 2:
            continue
        perm = []
        for a in range(nx):
            for b in range(ny):
                for c in range(nz):
                    place = [a, b, c]
                    p = place[axis]
                    partner = p ^ 1 if phase == 0 else (p + 1 if p % 2 else p - 1)
                    if 0 <= partner < sizes[axis]:
                        place[axis] = partner
                    elif axis == 1:
                        place[1] = ny - 1 - p
                    else:
                        place[1] ^= 1
                    source = (a * ny + b) * nz + c
                    perm.append((source, (place[0] * ny + place[1]) * nz + place[2]))
        swaps.append((axis, phase, perm))
    return swaps


def rounded(a):
    return a.astype(BF16).astype(F32)


def split3(a):
    high = rounded(a)
    rest = a - high
    mid = rounded(rest)
    return high, mid, rounded(rest - mid)


def row_ids(shape):
    return lax.broadcasted_iota(jnp.int32, shape, 0)


def pick_rows(rows, shape):
    ids = row_ids(shape)
    out = jnp.zeros(shape, F32)
    for s, r in enumerate(rows):
        out = jnp.where(ids == s, r, out)
    return out


def centre(shape):
    parts = [lax.axis_index(ax).astype(F32) * SIDE + 0.5 * SIDE for ax in AXES]
    return pick_rows(parts, shape)


def scaled(x, mid, unit):
    n = x.shape[1]
    full = jnp.concatenate([x[:3], jnp.zeros((5, n), F32)], axis=0)
    return (full - mid) * (1.0 / unit)


def receiver_matrix(u):
    h, m, l = split3(u)
    norm = 1.0 - jnp.sum(u * u, axis=0, keepdims=True)
    a, b, c = split3(norm)
    h, m, l = 2.0 * h, 2.0 * m, 2.0 * l
    one = jnp.ones_like(norm)
    tail = pick_rows([a, b, c, one, one, one], u.shape)
    return jnp.concatenate([h, h, h, m, m, l, tail, jnp.zeros_like(u)], axis=0).astype(BF16)


def source_matrices(u, valid=None):
    h, m, l = split3(u)
    norm = -jnp.sum(u * u, axis=0, keepdims=True)
    if valid is not None:
        norm = jnp.where(valid, norm, FAR)
    a, b, c = split3(norm)
    one = jnp.ones_like(norm)
    tail = pick_rows([one, one, one, a, b, c], u.shape)
    pair = jnp.concatenate([h, m, l, h, m, h, tail, jnp.zeros_like(u)], axis=0)
    ids = row_ids(u.shape)
    total = jnp.concatenate([jnp.where(ids == 3, 1.0, h), m, l], axis=0)
    return pair, total


def dot(a, b):
    return jnp.dot(a, b, preferred_element_type=F32)


def two_parts(w):
    return w, w - rounded(w)


def pad8(x):
    return jnp.concatenate([x, jnp.zeros((8 - x.shape[0], x.shape[1]), F32)], axis=0)


def gather_grid(x, index):
    tile = lax.shift_right_logical(index, 7)
    lane = lax.bitwise_and(index, LANES - 1)
    hits = [tile == r for r in range(1, x.shape[1] // LANES)]
    out = []
    for c in range(x.shape[0]):
        got = None
        for r in range(x.shape[1] // LANES):
            row = jnp.broadcast_to(x[c : c + 1, r * LANES : (r + 1) * LANES], (8, LANES))
            here = jnp.take_along_axis(row, lane, axis=1)
            got = here if got is None else jnp.where(hits[r - 1], here, got)
        out.append(got)
    return out


def write_faces(x, index_ref, send_refs):
    per = send_refs[0].shape[1] // LANES
    for g in range(index_ref.shape[0] // 8):
        got = gather_grid(x, index_ref[8 * g : 8 * g + 8, :])
        for r in range(8 * g, min(8 * g + 8, per * len(send_refs))):
            part = slice(r % per * LANES, (r % per + 1) * LANES)
            for c, rows in enumerate(got):
                send_refs[r // per][c : c + 1, part] = rows[r % 8 : r % 8 + 1]


def write_face_index(swaps, index_ref, out_ref):
    per = index_ref.shape[1] // LANES
    out_ref[...] = jnp.zeros_like(out_ref)
    for k, (axis, phase, _) in enumerate(swaps):
        even = lax.axis_index(AXES[axis]) % 2 == 0
        high = even if phase == 0 else jnp.logical_not(even)
        low_row, high_row = index_ref[2 * axis : 2 * axis + 1, :], index_ref[2 * axis + 1 : 2 * axis + 2, :]
        row = jnp.where(high, high_row, low_row)
        for w in range(per):
            out_ref[per * k + w : per * k + w + 1, :] = row[:, w * LANES : (w + 1) * LANES]


def write_grid(row_ref, out_ref):
    for t in range(out_ref.shape[1]):
        for e in range(out_ref.shape[0]):
            out_ref[e, t : t + 1, :] = row_ref[e : e + 1, t * LANES : (t + 1) * LANES]


def start_kernel(swaps, *refs):
    sources, refs = refs[:N_START], refs[N_START:]
    x_ref, mass_ref, charge_ref, partner_ref = refs[:4]
    index_out, bonds_out, bond_k_out, x_out, v_out = refs[4:9]
    send_refs, refs = refs[9 : 9 + len(swaps)], refs[9 + len(swaps) :]
    v_ref, fast_ref, slow_ref, index_ref, bonds_ref, bond_k_ref, sems = refs
    kept = [x_ref, mass_ref, index_ref, v_ref, fast_ref, slow_ref]
    kept += [charge_ref, bonds_ref, bond_k_ref, partner_ref]
    copies = [
        pltpu.make_async_copy(src, dst, sems.at[k]) for k, (src, dst) in enumerate(zip(sources, kept))
    ]
    for c in copies:
        c.start()
    for c in copies[:6]:
        c.wait()
    write_face_index(swaps, index_ref, index_out)
    mass = mass_ref[...]
    v = v_ref[...] + (0.5 * INNER * STEP) * mass * slow_ref[...]
    v = v + (0.5 * STEP) * mass * fast_ref[...]
    x = x_ref[...] + STEP * v
    x_out[...] = x
    v_out[...] = v
    write_faces(x, index_out, send_refs)
    for c in copies[6:]:
        c.wait()
    write_grid(bonds_ref, bonds_out)
    write_grid(bond_k_ref, bond_k_out)


def pair_sums(receivers, sources, totals, fold=None):
    sums = []
    for it in range(len(receivers)):
        out = None
        for st in range(len(sources)):
            closeness = dot(sources[st], receivers[it])
            high, low = two_parts(jnp.maximum(closeness, 0.0))
            part = dot(totals[st], high) + dot(totals[st], low)
            if fold is not None:
                part = fold(it, st, part)
            out = part if out is None else out + part
        sums.append(out)
    return sums


def short_from(u, sums):
    part = sums[0:8] + sums[8:16] + sums[16:24]
    return SHORT_UNIT * (u * part[3:4] - part)


def blocks(a, width=BLOCK):
    return [a[:, s : s + width] for s in range(0, a.shape[1], width)]


def tile_counts(own_ref, partner_ref, n_tiles, swaps):
    slots = partner_ref.shape[1]
    partner = partner_ref[...]
    own = own_ref[:, :slots]
    live = lax.broadcasted_iota(jnp.int32, (1, slots), 1) < own_ref[:, slots:]
    outside = partner - n_tiles
    axis = lax.shift_right_logical(outside, 2)
    side = lax.bitwise_and(lax.shift_right_logical(outside, 1), 1)
    within = lax.bitwise_and(outside, 1)
    place = jnp.full_like(partner, -1)
    for k, (ax, phase, _) in enumerate(swaps):
        even = lax.axis_index(AXES[ax]) % 2 == 0
        high = even if phase == 0 else jnp.logical_not(even)
        want = jnp.where(high, 1, 0)
        place = jnp.where((axis == ax) & (side == want), n_tiles + 2 * k + within, place)
    place = jnp.where(outside < 0, partner, place)
    own_hot = jnp.where((row_ids((8, slots)) == own) & live, 1.0, 0.0)
    place_hot = jnp.where(row_ids((32, slots)) == place, 1.0, 0.0)
    return lax.dot_general(own_hot, place_hot, (((1,), (1,)), ((), ())), preferred_element_type=F32)


def slow_totals(u, charge):
    base = jnp.where(row_ids(u.shape) == 3, 1.0, u) * charge
    rows = jnp.concatenate(split3(base), axis=0)
    first = lax.broadcasted_iota(jnp.int32, rows.shape, 1) < LANES
    return jnp.concatenate([jnp.where(first, rows, 0.0), jnp.where(first, 0.0, rows)], axis=0)


def slow_fold(counts, first_tile):
    wide = {}

    def row(it, u):
        if u not in wide:
            wide[u] = jnp.broadcast_to(counts[:, u : u + 1], (8, LANES))
        return jnp.concatenate([wide[u][2 * it : 2 * it + 1], wide[u][2 * it + 1 : 2 * it + 2]], axis=1)

    def fold(it, st, part):
        u = first_tile + 2 * st
        return part[:24] * row(it, u) + part[24:] * row(it, u + 1)

    return fold


def slow_from(u, charge, sums):
    part = sums[0:8] + sums[8:16] + sums[16:24]
    return (LONG_SCALE * LONG_UNIT) * charge * (u * part[3:4] - part)


def slow_own_kernel(swaps, x_ref, charge_ref, own_ref, partner_ref, slow_out, counts_out):
    n = x_ref.shape[1]
    charge = charge_ref[...]
    u = scaled(x_ref[...], centre((8, n)), LONG_UNIT)
    pair, _ = source_matrices(u)
    counts = tile_counts(own_ref, partner_ref, n // LANES, swaps)
    counts_out[...] = counts
    sums = pair_sums(
        blocks(receiver_matrix(u)),
        [jnp.transpose(p).astype(BF16) for p in blocks(pair)],
        [slow_totals(b, q) for b, q in zip(blocks(u), blocks(charge))],
        slow_fold(counts, 0),
    )
    slow_out[...] = slow_from(u, charge, jnp.concatenate(sums, axis=1))[:3]


def slow_halo_kernel(swaps, *refs):
    x_ref, v_ref, mass_ref, charge_ref, counts_ref, slow_ref, force_ref, start_ref = refs[:8]
    arrived, refs = refs[8 : 8 + len(swaps)], refs[8 + len(swaps) :]
    outs, (moved, v_new, slow_new, sems) = refs[:4], refs[4:]
    x = x_ref[...]
    n = x.shape[1]
    moved[...] = x - start_ref[...]
    copies = [
        pltpu.make_async_copy(src, dst, sems.at[k])
        for k, (src, dst) in enumerate(zip([moved, v_new, force_ref, slow_new], outs))
    ]
    u = scaled(x, centre((8, n)), LONG_UNIT)
    charge = charge_ref[...]
    sources, totals = [], []
    for swap, ref in zip(swaps, arrived):
        got = ref[...]
        there, valid = halo_place(swap, got, LONG_UNIT)
        sources.append(jnp.transpose(source_matrices(there, valid)[0]).astype(BF16))
        totals.append(slow_totals(there, got[3:4]))
    sums = pair_sums(
        blocks(receiver_matrix(u)), sources, totals, slow_fold(counts_ref[...], n // LANES)
    )
    slow = slow_ref[...] + slow_from(u, charge, jnp.concatenate(sums, axis=1))[:3]
    slow_new[...] = slow
    v_new[...] = v_ref[...] + (0.5 * INNER * STEP) * mass_ref[...] * slow
    for c in copies:
        c.start()
    for c in copies:
        c.wait()


def halo_place(swap, got, unit):
    axis, phase, _ = swap
    place = lax.axis_index(AXES[axis])
    valid = place >= 0
    if phase:
        valid = (place > 0) & (place < lax.axis_size(AXES[axis]) - 1)
    there = scaled(got, centre((8, got.shape[1])), unit)
    return jnp.where(valid, there, 0.0), valid


def own_kernel(first, *refs):
    x_ref, bonds_ref, bond_k_ref = refs[:3]
    out_ref, incidence = refs[3:] if first else (refs[4], refs[3])
    x = x_ref[...]
    n = x.shape[1]
    pulls = []
    for g in range(bonds_ref.shape[1] // 8):
        rows = slice(8 * g, 8 * g + 8)
        ends = zip(gather_grid(x, bonds_ref[0, rows, :]), gather_grid(x, bonds_ref[1, rows, :]))
        pull = [bond_k_ref[0, rows, :] * (i - j) for i, j in ends]
        for t in range(8):
            pulls.append(jnp.concatenate([p[t : t + 1] for p in pull], axis=0))
    pull = pad8(jnp.concatenate(pulls, axis=1))
    pull = jnp.concatenate(split3(pull), axis=0).astype(BF16)
    if first:
        for t in range(bonds_ref.shape[1]):
            part = slice(t * LANES, (t + 1) * LANES)
            i = jnp.transpose(jnp.broadcast_to(bonds_ref[0, t : t + 1, :], (LANES, LANES)))
            j = jnp.transpose(jnp.broadcast_to(bonds_ref[1, t : t + 1, :], (LANES, LANES)))
            for s in range(n // LANES):
                atom = lax.broadcasted_iota(jnp.int32, (LANES, LANES), 1) + s * LANES
                hit = jnp.where(j == atom, 1.0, 0.0)
                hit = jnp.where(i == atom, hit - 1.0, hit)
                incidence[part, s * LANES : (s + 1) * LANES] = hit.astype(BF16)
    bonded = dot(pull, incidence[...])
    bonded = bonded[0:8] + bonded[8:16] + bonded[16:24]

    u = scaled(x, centre((8, n)), SHORT_UNIT)
    pair, total = source_matrices(u)
    sums = pair_sums(
        blocks(receiver_matrix(u)),
        [jnp.transpose(p).astype(BF16) for p in blocks(pair)],
        blocks(total),
    )
    force = short_from(u, jnp.concatenate(sums, axis=1)) + bonded
    out_ref[...] = force[:3]


def halo_kernel(swaps, last, send_charge, *refs):
    x_ref, v_ref, mass_ref, force_ref = refs[:4]
    arrived, refs = refs[4 : 4 + len(swaps)], refs[4 + len(swaps) :]
    x = x_ref[...]
    u = scaled(x, centre((8, x.shape[1])), SHORT_UNIT)
    sources, totals = [], []
    for swap, ref in zip(swaps, arrived):
        pair, total = source_matrices(*halo_place(swap, ref[...], SHORT_UNIT))
        sources.append(jnp.transpose(pair).astype(BF16))
        totals.append(total)
    sums = pair_sums(blocks(receiver_matrix(u)), sources, totals)
    mass = mass_ref[...]
    force = force_ref[...] + short_from(u, jnp.concatenate(sums, axis=1))[:3]
    v = v_ref[...] + (0.5 * STEP) * mass * force
    if last:
        force_out, v_out = refs
        force_out[...] = force
        v_out[...] = v
        return
    index_ref, refs = refs[0], refs[1:]
    charge = None
    if send_charge:
        charge, refs = refs[0][...], refs[1:]
    v = v + (0.5 * STEP) * mass * force
    x = x + STEP * v
    refs[0][...] = x
    refs[1][...] = v
    if send_charge:
        x = jnp.concatenate([x, charge], axis=0)
    write_faces(x, index_ref, refs[2:])


def own_last_kernel(swaps, *refs):
    own_kernel(False, *refs[:4], refs[7])
    slow_own_kernel(swaps, refs[0], *refs[4:7], *refs[8:])


def halo_last_kernel(swaps, *refs):
    x_ref, v_ref, mass_ref, force_ref = refs[:4]
    arrived, refs = refs[4 : 4 + len(swaps)], refs[4 + len(swaps) :]
    charge_ref, counts_ref, slow_ref, start_ref = refs[:4]
    outs, (moved, v_new, slow_new, force_new, v_mid, sems) = refs[4:8], refs[8:]
    halo_kernel(swaps, True, False, x_ref, v_ref, mass_ref, force_ref, *arrived, force_new, v_mid)
    slow_halo_kernel(
        swaps, x_ref, v_mid, mass_ref, charge_ref, counts_ref, slow_ref, force_new, start_ref, *arrived, *outs,
        moved, v_new, slow_new, sems,
    )


def call(kernel, outs, args, flops=0):
    return pl.pallas_call(
        kernel,
        out_shape=[jax.ShapeDtypeStruct(s, d) for s, d in outs],
        in_specs=[pl.BlockSpec(memory_space=pltpu.VMEM)] * len(args),
        out_specs=[pl.BlockSpec(memory_space=pltpu.VMEM)] * len(outs),
        compiler_params=pltpu.CompilerParams(vmem_limit_bytes=24 * 1024 * 1024),
        cost_estimate=pl.CostEstimate(flops=flops, bytes_accessed=100000, transcendentals=0),
    )(*args)


def on_device(
    swaps,
    positions,
    velocities,
    inv_mass,
    charge,
    fast_force,
    slow_force,
    bonds,
    bond_k,
    halo_index,
    pair_own,
    pair_partner,
    pair_count,
):
    n = positions.shape[1]
    vec = ((3, n), F32)
    sends = [((4, halo_index.shape[1]), F32)] * len(swaps)
    start_args = [positions, inv_mass.reshape(1, n), halo_index, velocities, fast_force, slow_force]
    start_args += [charge.reshape(1, n), bonds, bond_k.reshape(1, -1)]
    start_args.append(pair_partner.reshape(1, -1))
    assert len(start_args) == N_START
    kept = [(start_args[k].shape, start_args[k].dtype) for k in (0, 1, 6, 9)]
    n_bonds = bonds.shape[1]
    face_rows = len(swaps) * halo_index.shape[1] // LANES
    kept.append(((-(-face_rows // 8) * 8, LANES), jnp.int32))
    kept.append(((2, n_bonds // LANES, LANES), jnp.int32))
    kept.append(((1, n_bonds // LANES, LANES), F32))
    scratch = [pltpu.VMEM((3, n), F32)] * 3
    scratch += [pltpu.VMEM(halo_index.shape, jnp.int32), pltpu.VMEM(bonds.shape, jnp.int32)]
    scratch += [pltpu.VMEM((1, n_bonds), F32), pltpu.SemaphoreType.DMA((N_START,))]
    start_args = [pltpu.with_memory_space_constraint(a, pltpu.HBM) for a in start_args]
    start, mass, charge, partner, index, bonds, bond_k, x, v, *faces = pl.pallas_call(
        functools.partial(start_kernel, swaps),
        out_shape=[jax.ShapeDtypeStruct(s, d) for s, d in kept + [vec, vec] + sends],
        in_specs=[pl.BlockSpec(memory_space=pltpu.HBM)] * N_START,
        out_specs=[pl.BlockSpec(memory_space=pltpu.VMEM)] * (len(kept) + 2 + len(sends)),
        scratch_shapes=scratch,
        compiler_params=pltpu.CompilerParams(vmem_limit_bytes=4 * 1024 * 1024),
    )(*start_args)
    incidence = None
    for turn in range(INNER):
        first, last = turn == 0, turn == INNER - 1
        arrived = [lax.ppermute(f, AXES, perm) for f, (_, _, perm) in zip(faces, swaps)]
        outs, args = [vec], [x, bonds, bond_k]
        if first:
            outs.append(((n_bonds, n), BF16))
        else:
            args.append(incidence)
        if last:
            own = jnp.concatenate([pair_own, pair_count]).reshape(1, -1)
            force, slow, counts = call(
                functools.partial(own_last_kernel, swaps),
                [vec, vec, ((8, 32), F32)],
                args + [charge, own, partner],
                flops=4 * 10**9,
            )
            break
        force, *built = call(functools.partial(own_kernel, first), outs, args, flops=2 * 10**9)
        if first:
            incidence = built[0]
        args = [x, v, mass, force] + arrived
        args.append(index)
        send_charge = turn == INNER - 2
        if send_charge:
            args.append(charge)
        x, v, *faces = call(
            functools.partial(halo_kernel, swaps, False, send_charge),
            [vec, vec] + sends,
            args,
            flops=10**9,
        )
    args = [x, v, mass, force] + arrived + [charge, counts, slow, start]
    return pl.pallas_call(
        functools.partial(halo_last_kernel, swaps),
        out_shape=[jax.ShapeDtypeStruct(*vec)] * 4,
        in_specs=[pl.BlockSpec(memory_space=pltpu.VMEM)] * len(args),
        out_specs=[pl.BlockSpec(memory_space=pltpu.HBM)] * 4,
        scratch_shapes=[pltpu.VMEM((3, n), F32)] * 5 + [pltpu.SemaphoreType.DMA((4,))],
        compiler_params=pltpu.CompilerParams(vmem_limit_bytes=24 * 1024 * 1024),
    )(*args)


def solution(mesh):
    rows = P(None, AXES)
    flat = P(AXES)
    swaps = matchings([mesh.shape[ax] for ax in AXES])
    return jax.shard_map(
        functools.partial(on_device, swaps),
        mesh=mesh,
        in_specs=(rows, rows, flat, flat, rows, rows, rows, flat, rows, flat, flat, flat),
        out_specs=(rows, rows, rows, rows),
        check_vma=False,
    )
```

```python
import functools

import jax
import jax.numpy as jnp
from jax import lax
from jax.experimental import pallas as pl
from jax.experimental.pallas import tpu as pltpu
from jax.sharding import PartitionSpec as P

AXES = ("gx", "gy", "gz")
INNER = 4
STEP = 0.1
LONG_SCALE = 0.5
SIDE = 4.0
SHORT_UNIT = 0.8
LONG_UNIT = 1.2
LANES = 128
BLOCK = 256
FAR = -1.0e6

N_START = 10
F32 = jnp.float32
BF16 = jnp.bfloat16


def matchings(sizes):
    nx, ny, nz = sizes
    assert nx % 2 == 0 and ny % 2 == 0 and nz % 2 == 0
    swaps = []
    for axis, phase in ((2, 0), (2, 1), (1, 1), (0, 0), (0, 1), (1, 0)):
        if phase and sizes[axis] == 2:
            continue
        perm = []
        for a in range(nx):
            for b in range(ny):
                for c in range(nz):
                    place = [a, b, c]
                    p = place[axis]
                    partner = p ^ 1 if phase == 0 else (p + 1 if p % 2 else p - 1)
                    if 0 <= partner < sizes[axis]:
                        place[axis] = partner
                    elif axis == 1:
                        place[1] = ny - 1 - p
                    else:
                        place[1] ^= 1
                    source = (a * ny + b) * nz + c
                    perm.append((source, (place[0] * ny + place[1]) * nz + place[2]))
        swaps.append((axis, phase, perm))
    return swaps


def rounded(a):
    return a.astype(BF16).astype(F32)


def split3(a):
    high = rounded(a)
    rest = a - high
    mid = rounded(rest)
    return high, mid, rounded(rest - mid)


def row_ids(shape):
    return lax.broadcasted_iota(jnp.int32, shape, 0)


def pick_rows(rows, shape):
    ids = row_ids(shape)
    out = jnp.zeros(shape, F32)
    for s, r in enumerate(rows):
        out = jnp.where(ids == s, r, out)
    return out


def centre(shape):
    parts = [lax.axis_index(ax).astype(F32) * SIDE + 0.5 * SIDE for ax in AXES]
    return pick_rows(parts, shape)


def scaled(x, mid, unit):
    n = x.shape[1]
    full = jnp.concatenate([x[:3], jnp.zeros((5, n), F32)], axis=0)
    return (full - mid) * (1.0 / unit)


def receiver_matrix(u):
    h, m, l = split3(u)
    norm = 1.0 - jnp.sum(u * u, axis=0, keepdims=True)
    a, b, c = split3(norm)
    h, m, l = 2.0 * h, 2.0 * m, 2.0 * l
    one = jnp.ones_like(norm)
    tail = pick_rows([a, b, c, one, one, one], u.shape)
    return jnp.concatenate([h, h, h, m, m, l, tail, jnp.zeros_like(u)], axis=0).astype(BF16)


def source_matrices(u, valid=None):
    h, m, l = split3(u)
    norm = -jnp.sum(u * u, axis=0, keepdims=True)
    if valid is not None:
        norm = jnp.where(valid, norm, FAR)
    a, b, c = split3(norm)
    one = jnp.ones_like(norm)
    tail = pick_rows([one, one, one, a, b, c], u.shape)
    pair = jnp.concatenate([h, m, l, h, m, h, tail, jnp.zeros_like(u)], axis=0)
    ids = row_ids(u.shape)
    total = jnp.concatenate([jnp.where(ids == 3, 1.0, h), m, l], axis=0)
    return pair, total


def dot(a, b):
    return jnp.dot(a, b, preferred_element_type=F32)


def two_parts(w, kind):
    if kind == F32:
        return w, w - rounded(w)
    high = w.astype(BF16)
    return high, (w - high.astype(F32)).astype(BF16)


def pad8(x):
    return jnp.concatenate([x, jnp.zeros((8 - x.shape[0], x.shape[1]), F32)], axis=0)


def gather_grid(x, index):
    tile = lax.shift_right_logical(index, 7)
    lane = lax.bitwise_and(index, LANES - 1)
    hits = [tile == r for r in range(1, x.shape[1] // LANES)]
    out = []
    for c in range(x.shape[0]):
        got = None
        for r in range(x.shape[1] // LANES):
            row = jnp.broadcast_to(x[c : c + 1, r * LANES : (r + 1) * LANES], (8, LANES))
            here = jnp.take_along_axis(row, lane, axis=1)
            got = here if got is None else jnp.where(hits[r - 1], here, got)
        out.append(got)
    return out


def write_faces(x, index_ref, send_refs):
    per = send_refs[0].shape[1] // LANES
    for g in range(index_ref.shape[0] // 8):
        got = gather_grid(x, index_ref[8 * g : 8 * g + 8, :])
        for r in range(8 * g, min(8 * g + 8, per * len(send_refs))):
            part = slice(r % per * LANES, (r % per + 1) * LANES)
            for c, rows in enumerate(got):
                send_refs[r // per][c : c + 1, part] = rows[r % 8 : r % 8 + 1]


def write_face_index(swaps, index_ref, out_ref):
    per = index_ref.shape[1] // LANES
    out_ref[...] = jnp.zeros_like(out_ref)
    for k, (axis, phase, _) in enumerate(swaps):
        even = lax.axis_index(AXES[axis]) % 2 == 0
        high = even if phase == 0 else jnp.logical_not(even)
        low_row, high_row = index_ref[2 * axis : 2 * axis + 1, :], index_ref[2 * axis + 1 : 2 * axis + 2, :]
        row = jnp.where(high, high_row, low_row)
        for w in range(per):
            out_ref[per * k + w : per * k + w + 1, :] = row[:, w * LANES : (w + 1) * LANES]


def write_grid(row_ref, out_ref):
    for t in range(out_ref.shape[1]):
        for e in range(out_ref.shape[0]):
            out_ref[e, t : t + 1, :] = row_ref[e : e + 1, t * LANES : (t + 1) * LANES]


def start_kernel(swaps, *refs):
    sources, refs = refs[:N_START], refs[N_START:]
    x_ref, mass_ref, charge_ref, partner_ref = refs[:4]
    index_out, bonds_out, bond_k_out, x_out, v_out = refs[4:9]
    send_refs, refs = refs[9 : 9 + len(swaps)], refs[9 + len(swaps) :]
    v_ref, fast_ref, slow_ref, index_ref, bonds_ref, bond_k_ref, sems = refs
    kept = [x_ref, mass_ref, index_ref, v_ref, fast_ref, slow_ref]
    kept += [charge_ref, bonds_ref, bond_k_ref, partner_ref]
    copies = [
        pltpu.make_async_copy(src, dst, sems.at[k]) for k, (src, dst) in enumerate(zip(sources, kept))
    ]
    for c in copies:
        c.start()
    for c in copies[:6]:
        c.wait()
    write_face_index(swaps, index_ref, index_out)
    mass = mass_ref[...]
    v = v_ref[...] + (0.5 * INNER * STEP) * mass * slow_ref[...]
    v = v + (0.5 * STEP) * mass * fast_ref[...]
    x = x_ref[...] + STEP * v
    x_out[...] = x
    v_out[...] = v
    write_faces(x, index_out, send_refs)
    for c in copies[6:]:
        c.wait()
    write_grid(bonds_ref, bonds_out)
    write_grid(bond_k_ref, bond_k_out)


def pair_sums(receivers, sources, totals, fold=None):
    sums = []
    for it in range(len(receivers)):
        out = None
        for st in range(len(sources)):
            closeness = dot(sources[st], receivers[it])
            high, low = two_parts(jnp.maximum(closeness, 0.0), totals[st].dtype)
            part = dot(totals[st], high) + dot(totals[st], low)
            if fold is not None:
                part = fold(it, st, part)
            out = part if out is None else out + part
        sums.append(out)
    return sums


def short_from(u, sums):
    part = sums[0:8] + sums[8:16] + sums[16:24]
    return SHORT_UNIT * (u * part[3:4] - part)


def blocks(a, width=BLOCK):
    return [a[:, s : s + width] for s in range(0, a.shape[1], width)]


def tile_counts(own_ref, partner_ref, n_tiles, swaps):
    slots = partner_ref.shape[1]
    partner = partner_ref[...]
    own = own_ref[:, :slots]
    live = lax.broadcasted_iota(jnp.int32, (1, slots), 1) < own_ref[:, slots:]
    outside = partner - n_tiles
    axis = lax.shift_right_logical(outside, 2)
    side = lax.bitwise_and(lax.shift_right_logical(outside, 1), 1)
    within = lax.bitwise_and(outside, 1)
    place = jnp.full_like(partner, -1)
    for k, (ax, phase, _) in enumerate(swaps):
        even = lax.axis_index(AXES[ax]) % 2 == 0
        high = even if phase == 0 else jnp.logical_not(even)
        want = jnp.where(high, 1, 0)
        place = jnp.where((axis == ax) & (side == want), n_tiles + 2 * k + within, place)
    place = jnp.where(outside < 0, partner, place)
    own_hot = jnp.where((row_ids((8, slots)) == own) & live, 1.0, 0.0)
    place_hot = jnp.where(row_ids((32, slots)) == place, 1.0, 0.0)
    return lax.dot_general(own_hot, place_hot, (((1,), (1,)), ((), ())), preferred_element_type=F32)


def slow_totals(u, charge):
    base = jnp.where(row_ids(u.shape) == 3, 1.0, u) * charge
    rows = jnp.concatenate(split3(base), axis=0)
    first = lax.broadcasted_iota(jnp.int32, rows.shape, 1) < LANES
    return jnp.concatenate([jnp.where(first, rows, 0.0), jnp.where(first, 0.0, rows)], axis=0)


def slow_fold(counts, first_tile):
    wide = {}

    def row(it, u):
        if u not in wide:
            wide[u] = jnp.broadcast_to(counts[:, u : u + 1], (8, LANES))
        return jnp.concatenate([wide[u][2 * it : 2 * it + 1], wide[u][2 * it + 1 : 2 * it + 2]], axis=1)

    def fold(it, st, part):
        u = first_tile + 2 * st
        return part[:24] * row(it, u) + part[24:] * row(it, u + 1)

    return fold


def slow_from(u, charge, sums):
    part = sums[0:8] + sums[8:16] + sums[16:24]
    return (LONG_SCALE * LONG_UNIT) * charge * (u * part[3:4] - part)


def slow_own_kernel(swaps, x_ref, charge_ref, own_ref, partner_ref, slow_out, counts_out):
    n = x_ref.shape[1]
    charge = charge_ref[...]
    u = scaled(x_ref[...], centre((8, n)), LONG_UNIT)
    pair, _ = source_matrices(u)
    counts = tile_counts(own_ref, partner_ref, n // LANES, swaps)
    counts_out[...] = counts
    sums = pair_sums(
        blocks(receiver_matrix(u)),
        [jnp.transpose(p).astype(BF16) for p in blocks(pair)],
        [slow_totals(b, q) for b, q in zip(blocks(u), blocks(charge))],
        slow_fold(counts, 0),
    )
    slow_out[...] = slow_from(u, charge, jnp.concatenate(sums, axis=1))[:3]


def slow_halo_kernel(swaps, *refs):
    x_ref, v_ref, mass_ref, charge_ref, counts_ref, slow_ref, force_ref, start_ref = refs[:8]
    arrived, refs = refs[8 : 8 + len(swaps)], refs[8 + len(swaps) :]
    outs, (moved, v_new, slow_new, sems) = refs[:4], refs[4:]
    x = x_ref[...]
    n = x.shape[1]
    moved[...] = x - start_ref[...]
    copies = [
        pltpu.make_async_copy(src, dst, sems.at[k])
        for k, (src, dst) in enumerate(zip([moved, v_new, force_ref, slow_new], outs))
    ]
    u = scaled(x, centre((8, n)), LONG_UNIT)
    charge = charge_ref[...]
    sources, totals = [], []
    for swap, ref in zip(swaps, arrived):
        got = ref[...]
        there, valid = halo_place(swap, got, LONG_UNIT)
        sources.append(jnp.transpose(source_matrices(there, valid)[0]).astype(BF16))
        totals.append(slow_totals(there, got[3:4]))
    sums = pair_sums(
        blocks(receiver_matrix(u)), sources, totals, slow_fold(counts_ref[...], n // LANES)
    )
    slow = slow_ref[...] + slow_from(u, charge, jnp.concatenate(sums, axis=1))[:3]
    slow_new[...] = slow
    v_new[...] = v_ref[...] + (0.5 * INNER * STEP) * mass_ref[...] * slow
    for c in copies:
        c.start()
    for c in copies:
        c.wait()


def halo_place(swap, got, unit):
    axis, phase, _ = swap
    place = lax.axis_index(AXES[axis])
    valid = place >= 0
    if phase:
        valid = (place > 0) & (place < lax.axis_size(AXES[axis]) - 1)
    there = scaled(got, centre((8, got.shape[1])), unit)
    return jnp.where(valid, there, 0.0), valid


def own_kernel(first, kind, *refs):
    x_ref, bonds_ref, bond_k_ref = refs[:3]
    out_ref, incidence = refs[3:] if first else (refs[4], refs[3])
    x = x_ref[...]
    n = x.shape[1]
    pulls = []
    for g in range(bonds_ref.shape[1] // 8):
        rows = slice(8 * g, 8 * g + 8)
        ends = zip(gather_grid(x, bonds_ref[0, rows, :]), gather_grid(x, bonds_ref[1, rows, :]))
        pull = [bond_k_ref[0, rows, :] * (i - j) for i, j in ends]
        for t in range(8):
            pulls.append(jnp.concatenate([p[t : t + 1] for p in pull], axis=0))
    pull = pad8(jnp.concatenate(pulls, axis=1))
    pull = jnp.concatenate(split3(pull), axis=0).astype(BF16)
    if first:
        for t in range(bonds_ref.shape[1]):
            part = slice(t * LANES, (t + 1) * LANES)
            i = jnp.transpose(jnp.broadcast_to(bonds_ref[0, t : t + 1, :], (LANES, LANES)))
            j = jnp.transpose(jnp.broadcast_to(bonds_ref[1, t : t + 1, :], (LANES, LANES)))
            for s in range(n // LANES):
                atom = lax.broadcasted_iota(jnp.int32, (LANES, LANES), 1) + s * LANES
                hit = jnp.where(j == atom, 1.0, 0.0)
                hit = jnp.where(i == atom, hit - 1.0, hit)
                incidence[part, s * LANES : (s + 1) * LANES] = hit.astype(BF16)
    bonded = dot(pull, incidence[...])
    bonded = bonded[0:8] + bonded[8:16] + bonded[16:24]

    u = scaled(x, centre((8, n)), SHORT_UNIT)
    pair, total = source_matrices(u)
    sums = pair_sums(
        blocks(receiver_matrix(u)),
        [jnp.transpose(p).astype(BF16) for p in blocks(pair)],
        blocks(total.astype(kind)),
    )
    force = short_from(u, jnp.concatenate(sums, axis=1)) + bonded
    out_ref[...] = force[:3]


def halo_kernel(swaps, last, send_charge, kind, *refs):
    x_ref, v_ref, mass_ref, force_ref = refs[:4]
    arrived, refs = refs[4 : 4 + len(swaps)], refs[4 + len(swaps) :]
    x = x_ref[...]
    u = scaled(x, centre((8, x.shape[1])), SHORT_UNIT)
    sources, totals = [], []
    for swap, ref in zip(swaps, arrived):
        pair, total = source_matrices(*halo_place(swap, ref[...], SHORT_UNIT))
        sources.append(jnp.transpose(pair).astype(BF16))
        totals.append(total.astype(kind))
    sums = pair_sums(blocks(receiver_matrix(u)), sources, totals)
    mass = mass_ref[...]
    force = force_ref[...] + short_from(u, jnp.concatenate(sums, axis=1))[:3]
    v = v_ref[...] + (0.5 * STEP) * mass * force
    if last:
        force_out, v_out = refs
        force_out[...] = force
        v_out[...] = v
        return
    index_ref, refs = refs[0], refs[1:]
    charge = None
    if send_charge:
        charge, refs = refs[0][...], refs[1:]
    v = v + (0.5 * STEP) * mass * force
    x = x + STEP * v
    refs[0][...] = x
    refs[1][...] = v
    if send_charge:
        x = jnp.concatenate([x, charge], axis=0)
    write_faces(x, index_ref, refs[2:])


def own_last_kernel(swaps, *refs):
    slow_own_kernel(swaps, refs[0], *refs[4:7], *refs[8:])
    own_kernel(False, F32, *refs[:4], refs[7])


def halo_last_kernel(swaps, *refs):
    x_ref, v_ref, mass_ref, force_ref = refs[:4]
    arrived, refs = refs[4 : 4 + len(swaps)], refs[4 + len(swaps) :]
    charge_ref, counts_ref, slow_ref, start_ref = refs[:4]
    outs, (moved, v_new, slow_new, force_new, v_mid, sems) = refs[4:8], refs[8:]
    halo_kernel(swaps, True, False, BF16, x_ref, v_ref, mass_ref, force_ref, *arrived, force_new, v_mid)
    slow_halo_kernel(
        swaps, x_ref, v_mid, mass_ref, charge_ref, counts_ref, slow_ref, force_new, start_ref, *arrived, *outs,
        moved, v_new, slow_new, sems,
    )


def call(kernel, outs, args, flops=0):
    return pl.pallas_call(
        kernel,
        out_shape=[jax.ShapeDtypeStruct(s, d) for s, d in outs],
        in_specs=[pl.BlockSpec(memory_space=pltpu.VMEM)] * len(args),
        out_specs=[pl.BlockSpec(memory_space=pltpu.VMEM)] * len(outs),
        compiler_params=pltpu.CompilerParams(vmem_limit_bytes=24 * 1024 * 1024),
        cost_estimate=pl.CostEstimate(flops=flops, bytes_accessed=100000, transcendentals=0),
    )(*args)


def on_device(
    swaps,
    positions,
    velocities,
    inv_mass,
    charge,
    fast_force,
    slow_force,
    bonds,
    bond_k,
    halo_index,
    pair_own,
    pair_partner,
    pair_count,
):
    n = positions.shape[1]
    vec = ((3, n), F32)
    sends = [((4, halo_index.shape[1]), F32)] * len(swaps)
    start_args = [positions, inv_mass.reshape(1, n), halo_index, velocities, fast_force, slow_force]
    start_args += [charge.reshape(1, n), bonds, bond_k.reshape(1, -1)]
    start_args.append(pair_partner.reshape(1, -1))
    assert len(start_args) == N_START
    kept = [(start_args[k].shape, start_args[k].dtype) for k in (0, 1, 6, 9)]
    n_bonds = bonds.shape[1]
    face_rows = len(swaps) * halo_index.shape[1] // LANES
    kept.append(((-(-face_rows // 8) * 8, LANES), jnp.int32))
    kept.append(((2, n_bonds // LANES, LANES), jnp.int32))
    kept.append(((1, n_bonds // LANES, LANES), F32))
    scratch = [pltpu.VMEM((3, n), F32)] * 3
    scratch += [pltpu.VMEM(halo_index.shape, jnp.int32), pltpu.VMEM(bonds.shape, jnp.int32)]
    scratch += [pltpu.VMEM((1, n_bonds), F32), pltpu.SemaphoreType.DMA((N_START,))]
    start_args = [pltpu.with_memory_space_constraint(a, pltpu.HBM) for a in start_args]
    start, mass, charge, partner, index, bonds, bond_k, x, v, *faces = pl.pallas_call(
        functools.partial(start_kernel, swaps),
        out_shape=[jax.ShapeDtypeStruct(s, d) for s, d in kept + [vec, vec] + sends],
        in_specs=[pl.BlockSpec(memory_space=pltpu.HBM)] * N_START,
        out_specs=[pl.BlockSpec(memory_space=pltpu.VMEM)] * (len(kept) + 2 + len(sends)),
        scratch_shapes=scratch,
        compiler_params=pltpu.CompilerParams(vmem_limit_bytes=4 * 1024 * 1024),
    )(*start_args)
    incidence = None
    for turn in range(INNER):
        first, last = turn == 0, turn == INNER - 1
        arrived = [lax.ppermute(f, AXES, perm) for f, (_, _, perm) in zip(faces, swaps)]
        outs, args = [vec], [x, bonds, bond_k]
        if first:
            outs.append(((n_bonds, n), BF16))
        else:
            args.append(incidence)
        if last:
            own = jnp.concatenate([pair_own, pair_count]).reshape(1, -1)
            force, slow, counts = call(
                functools.partial(own_last_kernel, swaps),
                [vec, vec, ((8, 32), F32)],
                args + [charge, own, partner],
                flops=4 * 10**9,
            )
            break
        force, *built = call(functools.partial(own_kernel, first, BF16), outs, args, flops=2 * 10**9)
        if first:
            incidence = built[0]
        args = [x, v, mass, force] + arrived
        args.append(index)
        send_charge = turn == INNER - 2
        if send_charge:
            args.append(charge)
        x, v, *faces = call(
            functools.partial(halo_kernel, swaps, False, send_charge, BF16),
            [vec, vec] + sends,
            args,
            flops=10**9,
        )
    args = [x, v, mass, force] + arrived + [charge, counts, slow, start]
    return pl.pallas_call(
        functools.partial(halo_last_kernel, swaps),
        out_shape=[jax.ShapeDtypeStruct(*vec)] * 4,
        in_specs=[pl.BlockSpec(memory_space=pltpu.VMEM)] * len(args),
        out_specs=[pl.BlockSpec(memory_space=pltpu.HBM)] * 4,
        scratch_shapes=[pltpu.VMEM((3, n), F32)] * 5 + [pltpu.SemaphoreType.DMA((4,))],
        compiler_params=pltpu.CompilerParams(vmem_limit_bytes=24 * 1024 * 1024),
    )(*args)


def solution(mesh):
    rows = P(None, AXES)
    flat = P(AXES)
    swaps = matchings([mesh.shape[ax] for ax in AXES])
    return jax.shard_map(
        functools.partial(on_device, swaps),
        mesh=mesh,
        in_specs=(rows, rows, flat, flat, rows, rows, rows, flat, rows, flat, flat, flat),
        out_specs=(rows, rows, rows, rows),
        check_vma=False,
    )
```

```python
import functools

import jax
import jax.numpy as jnp
from jax import lax
from jax.experimental import pallas as pl
from jax.experimental.pallas import tpu as pltpu
from jax.sharding import PartitionSpec as P

AXES = ("gx", "gy", "gz")
INNER = 4
STEP = 0.1
LONG_SCALE = 0.5
SIDE = 4.0
SHORT_UNIT = 0.8
LONG_UNIT = 1.2
LANES = 128
BLOCK = 256
FAR = -1.0e6

N_START = 10
F32 = jnp.float32
BF16 = jnp.bfloat16


def matchings(sizes):
    nx, ny, nz = sizes
    assert nx % 2 == 0 and ny % 2 == 0 and nz % 2 == 0
    swaps = []
    for axis, phase in ((2, 0), (2, 1), (1, 1), (0, 0), (0, 1), (1, 0)):
        if phase and sizes[axis] == 2:
            continue
        perm = []
        for a in range(nx):
            for b in range(ny):
                for c in range(nz):
                    place = [a, b, c]
                    p = place[axis]
                    partner = p ^ 1 if phase == 0 else (p + 1 if p % 2 else p - 1)
                    if 0 <= partner < sizes[axis]:
                        place[axis] = partner
                    elif axis == 1:
                        place[1] = ny - 1 - p
                    else:
                        place[1] ^= 1
                    source = (a * ny + b) * nz + c
                    perm.append((source, (place[0] * ny + place[1]) * nz + place[2]))
        swaps.append((axis, phase, perm))
    return swaps


def rounded(a):
    return a.astype(BF16).astype(F32)


def split3(a):
    high = rounded(a)
    rest = a - high
    mid = rounded(rest)
    return high, mid, rounded(rest - mid)


def row_ids(shape):
    return lax.broadcasted_iota(jnp.int32, shape, 0)


def pick_rows(rows, shape):
    ids = row_ids(shape)
    out = jnp.zeros(shape, F32)
    for s, r in enumerate(rows):
        out = jnp.where(ids == s, r, out)
    return out


def centre(shape):
    parts = [lax.axis_index(ax).astype(F32) * SIDE + 0.5 * SIDE for ax in AXES]
    return pick_rows(parts, shape)


def scaled(x, mid, unit):
    n = x.shape[1]
    full = jnp.concatenate([x[:3], jnp.zeros((5, n), F32)], axis=0)
    return (full - mid) * (1.0 / unit)


def receiver_matrix(u):
    h, m, l = split3(u)
    norm = 1.0 - jnp.sum(u * u, axis=0, keepdims=True)
    a, b, c = split3(norm)
    h, m, l = 2.0 * h, 2.0 * m, 2.0 * l
    one = jnp.ones_like(norm)
    tail = pick_rows([a, b, c, one, one, one], u.shape)
    return jnp.concatenate([h, h, h, m, m, l, tail, jnp.zeros_like(u)], axis=0).astype(BF16)


def source_matrices(u, valid=None):
    h, m, l = split3(u)
    norm = -jnp.sum(u * u, axis=0, keepdims=True)
    if valid is not None:
        norm = jnp.where(valid, norm, FAR)
    a, b, c = split3(norm)
    one = jnp.ones_like(norm)
    tail = pick_rows([one, one, one, a, b, c], u.shape)
    pair = jnp.concatenate([h, m, l, h, m, h, tail, jnp.zeros_like(u)], axis=0)
    ids = row_ids(u.shape)
    total = jnp.concatenate([jnp.where(ids == 3, 1.0, h), m, l], axis=0)
    return pair, total


def dot(a, b):
    return jnp.dot(a, b, preferred_element_type=F32)


def two_parts(w, kind):
    if kind == F32:
        return w, w - rounded(w)
    high = w.astype(BF16)
    return high, (w - high.astype(F32)).astype(BF16)


def pad8(x):
    return jnp.concatenate([x, jnp.zeros((8 - x.shape[0], x.shape[1]), F32)], axis=0)


def gather_grid(x, index):
    tile = lax.shift_right_logical(index, 7)
    lane = lax.bitwise_and(index, LANES - 1)
    hits = [tile == r for r in range(1, x.shape[1] // LANES)]
    out = []
    for c in range(x.shape[0]):
        got = None
        for r in range(x.shape[1] // LANES):
            row = jnp.broadcast_to(x[c : c + 1, r * LANES : (r + 1) * LANES], (8, LANES))
            here = jnp.take_along_axis(row, lane, axis=1)
            got = here if got is None else jnp.where(hits[r - 1], here, got)
        out.append(got)
    return out


def write_faces(x, index_ref, send_refs):
    per = send_refs[0].shape[1] // LANES
    for g in range(index_ref.shape[0] // 8):
        got = gather_grid(x, index_ref[8 * g : 8 * g + 8, :])
        for r in range(8 * g, min(8 * g + 8, per * len(send_refs))):
            part = slice(r % per * LANES, (r % per + 1) * LANES)
            for c, rows in enumerate(got):
                send_refs[r // per][c : c + 1, part] = rows[r % 8 : r % 8 + 1]


def write_face_index(swaps, index_ref, out_ref):
    per = index_ref.shape[1] // LANES
    out_ref[...] = jnp.zeros_like(out_ref)
    for k, (axis, phase, _) in enumerate(swaps):
        even = lax.axis_index(AXES[axis]) % 2 == 0
        high = even if phase == 0 else jnp.logical_not(even)
        low_row, high_row = index_ref[2 * axis : 2 * axis + 1, :], index_ref[2 * axis + 1 : 2 * axis + 2, :]
        row = jnp.where(high, high_row, low_row)
        for w in range(per):
            out_ref[per * k + w : per * k + w + 1, :] = row[:, w * LANES : (w + 1) * LANES]


def write_grid(row_ref, out_ref):
    for t in range(out_ref.shape[1]):
        for e in range(out_ref.shape[0]):
            out_ref[e, t : t + 1, :] = row_ref[e : e + 1, t * LANES : (t + 1) * LANES]


def start_kernel(swaps, *refs):
    sources, refs = refs[:N_START], refs[N_START:]
    x_ref, mass_ref, charge_ref, partner_ref = refs[:4]
    index_out, bonds_out, bond_k_out, x_out, v_out = refs[4:9]
    send_refs, refs = refs[9 : 9 + len(swaps)], refs[9 + len(swaps) :]
    v_ref, fast_ref, slow_ref, index_ref, bonds_ref, bond_k_ref, sems = refs
    kept = [x_ref, mass_ref, index_ref, v_ref, fast_ref, slow_ref]
    kept += [charge_ref, bonds_ref, bond_k_ref, partner_ref]
    copies = [
        pltpu.make_async_copy(src, dst, sems.at[k]) for k, (src, dst) in enumerate(zip(sources, kept))
    ]
    for c in copies:
        c.start()
    for c in copies[:6]:
        c.wait()
    write_face_index(swaps, index_ref, index_out)
    mass = mass_ref[...]
    v = v_ref[...] + (0.5 * INNER * STEP) * mass * slow_ref[...]
    v = v + (0.5 * STEP) * mass * fast_ref[...]
    x = x_ref[...] + STEP * v
    x_out[...] = x
    v_out[...] = v
    write_faces(x, index_out, send_refs)
    for c in copies[6:]:
        c.wait()
    write_grid(bonds_ref, bonds_out)
    write_grid(bond_k_ref, bond_k_out)


def pair_sums(receivers, sources, totals, fold=None):
    sums = []
    for it in range(len(receivers)):
        out = None
        for st in range(len(sources)):
            closeness = dot(sources[st], receivers[it])
            high, low = two_parts(jnp.maximum(closeness, 0.0), totals[st].dtype)
            part = dot(totals[st], high) + dot(totals[st], low)
            if fold is not None:
                part = fold(it, st, part)
            out = part if out is None else out + part
        sums.append(out)
    return sums


def short_from(u, sums):
    part = sums[0:8] + sums[8:16] + sums[16:24]
    return SHORT_UNIT * (u * part[3:4] - part)


def blocks(a, width=BLOCK):
    return [a[:, s : s + width] for s in range(0, a.shape[1], width)]


def tile_counts(own_ref, partner_ref, n_tiles, swaps):
    slots = partner_ref.shape[1]
    partner = partner_ref[...]
    own = own_ref[:, :slots]
    live = lax.broadcasted_iota(jnp.int32, (1, slots), 1) < own_ref[:, slots:]
    outside = partner - n_tiles
    axis = lax.shift_right_logical(outside, 2)
    side = lax.bitwise_and(lax.shift_right_logical(outside, 1), 1)
    within = lax.bitwise_and(outside, 1)
    place = jnp.full_like(partner, -1)
    for k, (ax, phase, _) in enumerate(swaps):
        even = lax.axis_index(AXES[ax]) % 2 == 0
        high = even if phase == 0 else jnp.logical_not(even)
        want = jnp.where(high, 1, 0)
        place = jnp.where((axis == ax) & (side == want), n_tiles + 2 * k + within, place)
    place = jnp.where(outside < 0, partner, place)
    own_hot = jnp.where((row_ids((8, slots)) == own) & live, 1.0, 0.0)
    place_hot = jnp.where(row_ids((32, slots)) == place, 1.0, 0.0)
    return lax.dot_general(own_hot, place_hot, (((1,), (1,)), ((), ())), preferred_element_type=F32)


def slow_totals(u, charge):
    base = jnp.where(row_ids(u.shape) == 3, 1.0, u) * charge
    rows = jnp.concatenate(split3(base), axis=0)
    first = lax.broadcasted_iota(jnp.int32, rows.shape, 1) < LANES
    return jnp.concatenate([jnp.where(first, rows, 0.0), jnp.where(first, 0.0, rows)], axis=0)


def slow_fold(counts, first_tile):
    wide = {}

    def row(it, u):
        if u not in wide:
            wide[u] = jnp.broadcast_to(counts[:, u : u + 1], (8, LANES))
        return jnp.concatenate([wide[u][2 * it : 2 * it + 1], wide[u][2 * it + 1 : 2 * it + 2]], axis=1)

    def fold(it, st, part):
        u = first_tile + 2 * st
        return part[:24] * row(it, u) + part[24:] * row(it, u + 1)

    return fold


def slow_from(u, charge, sums):
    part = sums[0:8] + sums[8:16] + sums[16:24]
    return (LONG_SCALE * LONG_UNIT) * charge * (u * part[3:4] - part)


def slow_own_kernel(swaps, x_ref, charge_ref, own_ref, partner_ref, slow_out, counts_out):
    n = x_ref.shape[1]
    charge = charge_ref[...]
    u = scaled(x_ref[...], centre((8, n)), LONG_UNIT)
    pair, _ = source_matrices(u)
    counts = tile_counts(own_ref, partner_ref, n // LANES, swaps)
    counts_out[...] = counts
    sums = pair_sums(
        blocks(receiver_matrix(u)),
        [jnp.transpose(p).astype(BF16) for p in blocks(pair)],
        [slow_totals(b, q) for b, q in zip(blocks(u), blocks(charge))],
        slow_fold(counts, 0),
    )
    slow_out[...] = slow_from(u, charge, jnp.concatenate(sums, axis=1))[:3]


def slow_halo_kernel(swaps, *refs):
    x_ref, v_ref, mass_ref, charge_ref, counts_ref, slow_ref, force_ref, start_ref = refs[:8]
    arrived, refs = refs[8 : 8 + len(swaps)], refs[8 + len(swaps) :]
    outs, (moved, v_new, slow_new, sems) = refs[:4], refs[4:]
    x = x_ref[...]
    n = x.shape[1]
    moved[...] = x - start_ref[...]
    copies = [
        pltpu.make_async_copy(src, dst, sems.at[k])
        for k, (src, dst) in enumerate(zip([moved, v_new, force_ref, slow_new], outs))
    ]
    u = scaled(x, centre((8, n)), LONG_UNIT)
    charge = charge_ref[...]
    sources, totals = [], []
    for swap, ref in zip(swaps, arrived):
        got = ref[...]
        there, valid = halo_place(swap, got, LONG_UNIT)
        sources.append(jnp.transpose(source_matrices(there, valid)[0]).astype(BF16))
        totals.append(slow_totals(there, got[3:4]))
    sums = pair_sums(
        blocks(receiver_matrix(u)), sources, totals, slow_fold(counts_ref[...], n // LANES)
    )
    slow = slow_ref[...] + slow_from(u, charge, jnp.concatenate(sums, axis=1))[:3]
    slow_new[...] = slow
    v_new[...] = v_ref[...] + (0.5 * INNER * STEP) * mass_ref[...] * slow
    for c in copies:
        c.start()
    for c in copies:
        c.wait()


def halo_place(swap, got, unit):
    axis, phase, _ = swap
    place = lax.axis_index(AXES[axis])
    valid = place >= 0
    if phase:
        valid = (place > 0) & (place < lax.axis_size(AXES[axis]) - 1)
    there = scaled(got, centre((8, got.shape[1])), unit)
    return jnp.where(valid, there, 0.0), valid


def own_kernel(first, kind, *refs):
    x_ref, bonds_ref, bond_k_ref = refs[:3]
    out_ref, incidence = refs[3:] if first else (refs[4], refs[3])
    x = x_ref[...]
    n = x.shape[1]
    pulls = []
    for g in range(bonds_ref.shape[1] // 8):
        rows = slice(8 * g, 8 * g + 8)
        ends = zip(gather_grid(x, bonds_ref[0, rows, :]), gather_grid(x, bonds_ref[1, rows, :]))
        pull = [bond_k_ref[0, rows, :] * (i - j) for i, j in ends]
        for t in range(8):
            pulls.append(jnp.concatenate([p[t : t + 1] for p in pull], axis=0))
    pull = pad8(jnp.concatenate(pulls, axis=1))
    pull = jnp.concatenate(split3(pull), axis=0).astype(BF16)
    if first:
        for t in range(bonds_ref.shape[1]):
            part = slice(t * LANES, (t + 1) * LANES)
            lane = lax.broadcasted_iota(jnp.int32, (LANES, LANES), 1).astype(F32).astype(BF16)
            marks, tiles = [], []
            for e in range(2):
                index = jnp.broadcast_to(bonds_ref[e, t : t + 1, :], (LANES, LANES))
                within = lax.bitwise_and(index, LANES - 1).astype(F32)
                within = jnp.transpose(within).astype(BF16)
                marks.append(jnp.where(within == lane, jnp.ones_like(lane), jnp.zeros_like(lane)))
                tile = lax.shift_right_logical(index, 7).astype(F32)
                tiles.append(jnp.transpose(tile).astype(BF16))
            for s in range(n // LANES):
                here = [
                    jnp.where(tile == jnp.full_like(tile, s), mark, jnp.zeros_like(mark))
                    for tile, mark in zip(tiles, marks)
                ]
                incidence[part, s * LANES : (s + 1) * LANES] = here[1] - here[0]
    bonded = dot(pull, incidence[...])
    bonded = bonded[0:8] + bonded[8:16] + bonded[16:24]

    u = scaled(x, centre((8, n)), SHORT_UNIT)
    pair, total = source_matrices(u)
    sums = pair_sums(
        blocks(receiver_matrix(u)),
        [jnp.transpose(p).astype(BF16) for p in blocks(pair)],
        blocks(total.astype(kind)),
    )
    force = short_from(u, jnp.concatenate(sums, axis=1)) + bonded
    out_ref[...] = force[:3]


def halo_kernel(swaps, last, send_charge, kind, *refs):
    x_ref, v_ref, mass_ref, force_ref = refs[:4]
    arrived, refs = refs[4 : 4 + len(swaps)], refs[4 + len(swaps) :]
    x = x_ref[...]
    u = scaled(x, centre((8, x.shape[1])), SHORT_UNIT)
    sources, totals = [], []
    for swap, ref in zip(swaps, arrived):
        pair, total = source_matrices(*halo_place(swap, ref[...], SHORT_UNIT))
        sources.append(jnp.transpose(pair).astype(BF16))
        totals.append(total.astype(kind))
    sums = pair_sums(blocks(receiver_matrix(u)), sources, totals)
    mass = mass_ref[...]
    force = force_ref[...] + short_from(u, jnp.concatenate(sums, axis=1))[:3]
    v = v_ref[...] + (0.5 * STEP) * mass * force
    if last:
        force_out, v_out = refs
        force_out[...] = force
        v_out[...] = v
        return
    index_ref, refs = refs[0], refs[1:]
    charge = None
    if send_charge:
        charge, refs = refs[0][...], refs[1:]
    v = v + (0.5 * STEP) * mass * force
    x = x + STEP * v
    refs[0][...] = x
    refs[1][...] = v
    if send_charge:
        x = jnp.concatenate([x, charge], axis=0)
    write_faces(x, index_ref, refs[2:])


def own_last_kernel(swaps, *refs):
    slow_own_kernel(swaps, refs[0], *refs[4:7], *refs[8:])
    own_kernel(False, F32, *refs[:4], refs[7])


def halo_last_kernel(swaps, *refs):
    x_ref, v_ref, mass_ref, force_ref = refs[:4]
    arrived, refs = refs[4 : 4 + len(swaps)], refs[4 + len(swaps) :]
    charge_ref, counts_ref, slow_ref, start_ref = refs[:4]
    outs, (moved, v_new, slow_new, force_new, v_mid, sems) = refs[4:8], refs[8:]
    halo_kernel(swaps, True, False, BF16, x_ref, v_ref, mass_ref, force_ref, *arrived, force_new, v_mid)
    slow_halo_kernel(
        swaps, x_ref, v_mid, mass_ref, charge_ref, counts_ref, slow_ref, force_new, start_ref, *arrived, *outs,
        moved, v_new, slow_new, sems,
    )


def call(kernel, outs, args, flops=0):
    return pl.pallas_call(
        kernel,
        out_shape=[jax.ShapeDtypeStruct(s, d) for s, d in outs],
        in_specs=[pl.BlockSpec(memory_space=pltpu.VMEM)] * len(args),
        out_specs=[pl.BlockSpec(memory_space=pltpu.VMEM)] * len(outs),
        compiler_params=pltpu.CompilerParams(vmem_limit_bytes=24 * 1024 * 1024),
        cost_estimate=pl.CostEstimate(flops=flops, bytes_accessed=100000, transcendentals=0),
    )(*args)


def on_device(
    swaps,
    positions,
    velocities,
    inv_mass,
    charge,
    fast_force,
    slow_force,
    bonds,
    bond_k,
    halo_index,
    pair_own,
    pair_partner,
    pair_count,
):
    n = positions.shape[1]
    vec = ((3, n), F32)
    sends = [((4, halo_index.shape[1]), F32)] * len(swaps)
    start_args = [positions, inv_mass.reshape(1, n), halo_index, velocities, fast_force, slow_force]
    start_args += [charge.reshape(1, n), bonds, bond_k.reshape(1, -1)]
    start_args.append(pair_partner.reshape(1, -1))
    assert len(start_args) == N_START
    kept = [(start_args[k].shape, start_args[k].dtype) for k in (0, 1, 6, 9)]
    n_bonds = bonds.shape[1]
    face_rows = len(swaps) * halo_index.shape[1] // LANES
    kept.append(((-(-face_rows // 8) * 8, LANES), jnp.int32))
    kept.append(((2, n_bonds // LANES, LANES), jnp.int32))
    kept.append(((1, n_bonds // LANES, LANES), F32))
    scratch = [pltpu.VMEM((3, n), F32)] * 3
    scratch += [pltpu.VMEM(halo_index.shape, jnp.int32), pltpu.VMEM(bonds.shape, jnp.int32)]
    scratch += [pltpu.VMEM((1, n_bonds), F32), pltpu.SemaphoreType.DMA((N_START,))]
    start_args = [pltpu.with_memory_space_constraint(a, pltpu.HBM) for a in start_args]
    start, mass, charge, partner, index, bonds, bond_k, x, v, *faces = pl.pallas_call(
        functools.partial(start_kernel, swaps),
        out_shape=[jax.ShapeDtypeStruct(s, d) for s, d in kept + [vec, vec] + sends],
        in_specs=[pl.BlockSpec(memory_space=pltpu.HBM)] * N_START,
        out_specs=[pl.BlockSpec(memory_space=pltpu.VMEM)] * (len(kept) + 2 + len(sends)),
        scratch_shapes=scratch,
        compiler_params=pltpu.CompilerParams(vmem_limit_bytes=4 * 1024 * 1024),
    )(*start_args)
    incidence = None
    for turn in range(INNER):
        first, last = turn == 0, turn == INNER - 1
        arrived = [lax.ppermute(f, AXES, perm) for f, (_, _, perm) in zip(faces, swaps)]
        outs, args = [vec], [x, bonds, bond_k]
        if first:
            outs.append(((n_bonds, n), BF16))
        else:
            args.append(incidence)
        if last:
            own = jnp.concatenate([pair_own, pair_count]).reshape(1, -1)
            force, slow, counts = call(
                functools.partial(own_last_kernel, swaps),
                [vec, vec, ((8, 32), F32)],
                args + [charge, own, partner],
                flops=4 * 10**9,
            )
            break
        force, *built = call(functools.partial(own_kernel, first, BF16), outs, args, flops=2 * 10**9)
        if first:
            incidence = built[0]
        args = [x, v, mass, force] + arrived
        args.append(index)
        send_charge = turn == INNER - 2
        if send_charge:
            args.append(charge)
        x, v, *faces = call(
            functools.partial(halo_kernel, swaps, False, send_charge, BF16),
            [vec, vec] + sends,
            args,
            flops=10**9,
        )
    args = [x, v, mass, force] + arrived + [charge, counts, slow, start]
    return pl.pallas_call(
        functools.partial(halo_last_kernel, swaps),
        out_shape=[jax.ShapeDtypeStruct(*vec)] * 4,
        in_specs=[pl.BlockSpec(memory_space=pltpu.VMEM)] * len(args),
        out_specs=[pl.BlockSpec(memory_space=pltpu.HBM)] * 4,
        scratch_shapes=[pltpu.VMEM((3, n), F32)] * 5 + [pltpu.SemaphoreType.DMA((4,))],
        compiler_params=pltpu.CompilerParams(vmem_limit_bytes=24 * 1024 * 1024),
    )(*args)


def solution(mesh):
    rows = P(None, AXES)
    flat = P(AXES)
    swaps = matchings([mesh.shape[ax] for ax in AXES])
    return jax.shard_map(
        functools.partial(on_device, swaps),
        mesh=mesh,
        in_specs=(rows, rows, flat, flat, rows, rows, rows, flat, rows, flat, flat, flat),
        out_specs=(rows, rows, rows, rows),
        check_vma=False,
    )
```
